256 devices in a mesh: beam: 32 (over x, y, core), grp: 8 (over z).
Axes of the slice: x: 4, y: 4, z: 8, core: 2. Of those that a mesh axis runs over, the one named last changes fastest.
Arguments:
- beam_data: bfloat16 [2, 16384, 256], P(None, 'beam', 'grp'), may hold values from -6 to 6
- window_count: int32 [256], P(('beam', 'grp')), may hold values from 1 to 8
- slot_owner: int32 [256, 8, 1], P(('beam', 'grp')), may hold values from 0 to 31; in each aligned block of 8 rows (0 to 7, 8 to 15, ..., all dimensions but the last counted through in order) at most 2 rows name the same one
- slot_window: int32 [256, 8], P(('beam', 'grp')), may hold values from 0 to 3
- grid_index: int32 [256, 4096], P(('beam', 'grp')), may hold values from 0 to 4095
Outputs:
- spectrum: float32 [256, 4096], P(('beam', 'grp'))
The draws below stay inside these ranges and needn't reach their ends.
Inputs may be any that keep to these rules, and one draw needn't show every extreme that they name: a user's slots 0 to window_count - 1 are live. `slot_owner`: among the 8 slots of the users of one device no owner is named more than 2 times, a bound that some block reaches.
All inputs are finite; a program needn't handle non-finite values.
Results may differ from the reference program's by a relative error of at most 0.0003.
Values may be sent and summed in bfloat16 or wider, within the bound.
A program may use at most 64 MiB of HBM per device.

```python
import math
import jax
import jax.numpy as jnp
import numpy as np
from jax import lax

WIN_BEAMS = 128
NOISE_DIM = 64
WIN_DEV = 4
SNAPS = 256
USER_DEV = 1
SLOTS = 8
GRID = 4096
OVERSAMPLE = 32
ITERS = 8
BEAMS = 16384
USERS = 256
CAP = 2
N_BEAM = 32


def with_ends(drawn, rng, low, largest):
    longest = drawn.shape.index(max(drawn.shape))
    spots = []
    for shift in (0, 1):
        where = [jax.random.randint(jax.random.fold_in(rng, axis), (), 0, length) for axis, length in enumerate(drawn.shape)]
        where[longest] = (where[longest] + shift) % drawn.shape[longest]
        spots.append(tuple(where))
    return drawn.at[spots[0]].set(low).at[spots[1]].set(largest)


def steps_of(own_key, extent, split, smallest, top_value):
    def one(axis_at, parts):
        heights = jax.random.uniform(jax.random.fold_in(jax.random.fold_in(own_key, 6), axis_at), (parts,), jnp.float32, smallest / len(split), top_value / len(split))
        return jnp.repeat(jnp.exp(heights), extent[axis_at] // parts).reshape((-1,) + (1,) * (len(extent) - axis_at - 1))

    gain = one(*split[0])
    for cut in split[1:]:
        gain = gain * one(*cut)
    return gain


def assign_block(own_key, own, number, rows, count, top, limit, skew):
    ranking = jax.random.permutation(own_key, count)
    crowded, common = shares(count, rows * top, limit, skew, True), shares(count, rows * top, limit, skew, False)
    places = jnp.arange(count)

    def named(tallies, offset_by):
        used = int((tallies > 0).sum())
        fixed = max(1, used // 4)
        moved = fixed + (places - fixed + offset_by * (used - fixed)) % max(1, count - fixed)
        return jnp.zeros((count,), jnp.int32).at[ranking[jnp.where(places < fixed, places, moved)]].set(jnp.asarray(tallies, jnp.int32))

    tallies = jnp.where(number % 4 == 0, named(crowded, number // 4), named(common, number - number // 4 - 1))
    mixed = jax.random.permutation(jax.random.fold_in(own, 3), count)
    donor, sink = mixed[0:count // 2 * 2:2], mixed[1:count // 2 * 2:2]
    room = jnp.minimum(tallies[donor] - 1, limit - tallies[sink]) // 2
    room = jnp.where((donor == ranking[0]) | (sink == ranking[0]) | (tallies[sink] == 0), 0, jnp.maximum(room, 0))
    moved = jax.random.randint(jax.random.fold_in(own, 4), (count // 2,), 0, 1 << 20) % (room + 1)
    tallies = tallies.at[donor].add(-moved).at[sink].add(moved)
    items = jnp.searchsorted(jnp.cumsum(tallies), jnp.arange(rows * top), side="right").astype(jnp.int32)
    grid = items.reshape(top, rows).T
    grid = grid[jax.random.permutation(jax.random.fold_in(own, 1), rows)]
    offset_by = jax.random.randint(jax.random.fold_in(own, 2), (rows, 1), 0, top)
    return jnp.take_along_axis(grid, (jnp.arange(top)[None, :] + offset_by) % top, axis=1)


def shares(count, total, bound, slope, full):
    portions = [(1 << 20) // math.isqrt(standing ** slope) + 1 for standing in range(1, count + 1)]
    largest = bound if full else min(bound, max(-(-total // count), total * portions[0] // sum(portions)))
    least = 1 if total - largest >= count - 1 else 0
    given, spare = [largest] + [least] * (count - 1), total - largest - least * (count - 1)
    while spare > 0:
        movable = [i for i in range(1, count) if given[i] < largest] or [i for i in range(1, count) if given[i] < bound]
        mass, remaining = sum([portions[i] for i in movable]), spare
        for i in movable:
            more = min(bound - given[i], max(1, remaining * portions[i] // mass), spare)
            given[i] = given[i] + more
            spare = spare - more
    return np.array(given)


def centred(stream_key, extent, spread, limit, split=(), kind=jnp.bfloat16):
    loudness = steps_of(stream_key, extent, split, -0.22, 0.18) if split else 1.0
    values = jax.random.normal(stream_key, extent, jnp.float32) * spread * loudness
    return jnp.minimum(jnp.maximum(values, -limit), limit).astype(kind)


def setup_inputs(seed: int = 0) -> dict:
    key_list = jax.random.split(jax.random.key(seed), 6)
    beam_data = centred(key_list[0], (2, BEAMS, SNAPS), 1.0, 6.0, ((1, 32), (2, 8)))
    window_count = with_ends(jax.random.randint(key_list[1], (USERS,), 1, SLOTS + 1), jax.random.fold_in(key_list[1], 1), 1, SLOTS).astype(jnp.int32)
    slot_owner_keys = jax.random.split(jax.random.fold_in(key_list[2], 1), USERS * SLOTS // (USER_DEV * SLOTS))
    slot_owner_turns = jax.random.permutation(jax.random.fold_in(key_list[2], 3), USERS * SLOTS // (USER_DEV * SLOTS))
    slot_owner = jax.vmap(lambda own, number: assign_block(jax.random.fold_in(key_list[2], 2), own, number, USER_DEV * SLOTS, N_BEAM, 1, CAP, 2))(slot_owner_keys, slot_owner_turns).reshape((USERS, SLOTS, 1))
    slot_window = with_ends(jax.random.randint(key_list[3], (USERS, SLOTS), 0, WIN_DEV), jax.random.fold_in(key_list[3], 1), 0, WIN_DEV - 1).astype(jnp.int32)
    grid_index = with_ends(jax.random.randint(key_list[4], (USERS, GRID), 0, WIN_BEAMS * OVERSAMPLE), jax.random.fold_in(key_list[4], 1), 0, (WIN_BEAMS * OVERSAMPLE) - 1).astype(jnp.int32)
    return {"beam_data": beam_data, "window_count": window_count, "slot_owner": slot_owner, "slot_window": slot_window, "grid_index": grid_index}


highest = lax.Precision.HIGHEST
shift_factor = 1.05
spectral_floor = 0.05

def orthonormal(image_block):
    gram_matrix = jnp.dot(image_block.T.astype(jnp.float32), image_block.astype(jnp.float32), precision=highest, preferred_element_type=jnp.float32)
    lower_factor = jnp.linalg.cholesky(gram_matrix)
    return jax.scipy.linalg.solve_triangular(lower_factor, image_block.T, lower=True).T

def steering(grid_row, beams_total):
    position = (grid_row.astype(jnp.float32) + 0.5) / OVERSAMPLE
    offset = position[..., None] - jnp.arange(WIN_BEAMS, dtype=jnp.float32)
    turned = jnp.pi * offset
    magnitude = jnp.sin(turned) / (beams_total * jnp.sin(turned / beams_total))
    phase_angle = turned * ((beams_total - 1) / beams_total)
    return jnp.concatenate([magnitude * jnp.cos(phase_angle), magnitude * jnp.sin(phase_angle)], axis=-1)

def reference(beam_data, window_count, slot_owner, slot_window, grid_index):
    windows_all = BEAMS // WIN_BEAMS
    window_view = beam_data.astype(jnp.float32).reshape(2, windows_all, WIN_BEAMS, SNAPS)

    def window_gram(window_pair):
        real_part, imag_part = window_pair
        same_part = jnp.dot(real_part.astype(jnp.float32), real_part.T.astype(jnp.float32), precision=highest, preferred_element_type=jnp.float32)
        same_part = same_part + jnp.dot(imag_part.astype(jnp.float32), imag_part.T.astype(jnp.float32), precision=highest, preferred_element_type=jnp.float32)
        cross_part = jnp.dot(imag_part.astype(jnp.float32), real_part.T.astype(jnp.float32), precision=highest, preferred_element_type=jnp.float32)
        return (same_part, cross_part)
    grams_same, grams_cross = lax.map(window_gram, (window_view[0], window_view[1]))
    window = (slot_owner[:, :, 0] * WIN_DEV + slot_window).astype(jnp.int32)

    def per_user(user_item):
        count_live, window_row, grid_row = user_item
        live_mask = (jnp.arange(SLOTS, dtype=jnp.int32) < count_live).astype(jnp.float32)
        real_sum = jnp.einsum('k,kij->ij', live_mask, grams_same[window_row], precision=highest)
        cross_sum = jnp.einsum('k,kij->ij', live_mask, grams_cross[window_row], precision=highest)
        imag_sum = cross_sum - cross_sum.T
        inverse_count = 1.0 / (count_live.astype(jnp.float32) * SNAPS)
        covariance = jnp.concatenate([jnp.concatenate([real_sum, -imag_sum], axis=1), jnp.concatenate([imag_sum, real_sum], axis=1)], axis=0) * inverse_count
        square = jnp.dot(covariance.astype(jnp.float32), covariance.astype(jnp.float32), precision=highest, preferred_element_type=jnp.float32)
        fourth = jnp.dot(square.astype(jnp.float32), square.astype(jnp.float32), precision=highest, preferred_element_type=jnp.float32)
        shift_value = shift_factor * jnp.sqrt(jnp.sqrt(jnp.sqrt(jnp.sum(fourth * fourth))))
        shifted = shift_value * jnp.eye(2 * WIN_BEAMS, dtype=jnp.float32) - covariance
        start_block = jnp.concatenate([shifted[:, :NOISE_DIM], shifted[:, WIN_BEAMS:WIN_BEAMS + NOISE_DIM]], axis=1)
        noise_basis = orthonormal(start_block)
        for sweep in range(ITERS - 1):
            noise_basis = orthonormal(jnp.dot(shifted.astype(jnp.float32), noise_basis.astype(jnp.float32), precision=highest, preferred_element_type=jnp.float32))
        steering_rows = steering(grid_row, BEAMS)
        projected = jnp.dot(steering_rows.astype(jnp.float32), noise_basis.astype(jnp.float32), precision=highest, preferred_element_type=jnp.float32)
        leakage = lax.optimization_barrier(jnp.sum(projected * projected, axis=-1)) / lax.optimization_barrier(jnp.sum(steering_rows * steering_rows, axis=-1))
        return 1.0 / (leakage + spectral_floor)
    return lax.map(per_user, (window_count, window, grid_index))
```

```python
import functools

import jax
import jax.numpy as jnp
from jax import lax
from jax.experimental import pallas as pl
from jax.experimental.pallas import tpu as pltpu
from jax.sharding import PartitionSpec as P

WIN_BEAMS = 128
NOISE_DIM = 64
SNAPS = 256
OVERSAMPLE = 32
ITERS = 8


highest = lax.Precision.HIGHEST
shift_factor = 1.05
spectral_floor = 0.05


def total_of_pieces(value, axis):
    blocks = lax.all_gather(value, axis)
    return blocks.sum(axis=0)


def owner_slots(owners, locals_flat, beam_count, slot_cap):
    owner_hits = (owners[:, None] == jnp.arange(beam_count, dtype=jnp.int32)[None, :]).astype(
        jnp.int32
    )
    earlier = jnp.cumsum(owner_hits, axis=0) - owner_hits
    order_in = jnp.sum(earlier * owner_hits, axis=1)
    slot_match = owner_hits[:, :, None] * (
        order_in[:, None, None] == jnp.arange(slot_cap, dtype=jnp.int32)[None, None, :]
    ).astype(jnp.int32)
    requests = jnp.sum(slot_match * locals_flat[:, None, None], axis=0)
    return (requests, owners * slot_cap + order_in)


def pack_upper(same_part, imag_part):
    width = same_part.shape[-1]
    row_ids = jnp.arange(width, dtype=jnp.int32)[:, None]
    col_ids = jnp.arange(width, dtype=jnp.int32)[None, :]
    return jnp.where((row_ids <= col_ids)[None], same_part, imag_part)


def local_grams(window_view):
    same_part = jnp.einsum(
        "wis,wjs->wij", window_view[0], window_view[0], preferred_element_type=jnp.float32
    )
    same_part = same_part + jnp.einsum(
        "wis,wjs->wij", window_view[1], window_view[1], preferred_element_type=jnp.float32
    )
    cross_part = jnp.einsum(
        "wis,wjs->wij", window_view[1], window_view[0], preferred_element_type=jnp.float32
    )
    return (same_part, cross_part)


GROW = (3.4445, -4.7750, 2.0315)
CLOSE = ((3.109266, -3.792034, 1.535381), (1.90467, -1.282586, 0.3782733), (1.875, -1.25, 0.375))
EXTRA = 6
CHUNK = 512


def halves(value):
    high = value.astype(jnp.bfloat16)
    return high, (value - high.astype(jnp.float32)).astype(jnp.bfloat16)


def dot(left, right):
    return jnp.dot(left, right, preferred_element_type=jnp.float32)


def dot_nt(left, right):
    return lax.dot_general(
        left, right, (((1,), (1,)), ((), ())), preferred_element_type=jnp.float32
    )


def product(left, right):
    return dot(left[0], right[0]) + (dot(left[0], right[1]) + dot(left[1], right[0]))


def product_half(left, right):
    both = dot(
        jnp.concatenate([left[0], left[1]], axis=1),
        jnp.concatenate([right[0], right[0]], axis=0),
    )
    return both + dot(left[0], right[1])


def whole(top):
    n = WIN_BEAMS
    return jnp.concatenate([top, jnp.concatenate([-top[:, n:], top[:, :n]], axis=1)], axis=0)


def finish_kernel(beams_total, packed_ref, count_ref, grid_ref, out_ref, a_hi, a_lo, w_ref):
    n = WIN_BEAMS
    row = lax.broadcasted_iota(jnp.int32, (n, n), 0)
    col = lax.broadcasted_iota(jnp.int32, (n, n), 1)
    packed = packed_ref[...]
    flipped = packed.T
    same = jnp.where(row <= col, packed, flipped)
    imag = jnp.where(row > col, packed, jnp.where(row < col, -flipped, 0.0))
    scale = jnp.full((1, 1), 1.0, jnp.float32) / (count_ref[0].astype(jnp.float32) * SNAPS)
    top = jnp.concatenate([same, -imag], axis=1) * scale
    square = product(halves(top), halves(whole(top)))
    fourth = product(halves(square), halves(whole(square)))
    power = 2.0 * jnp.sum(fourth * fourth, axis=(0, 1), keepdims=True)
    shift = shift_factor * jnp.sqrt(jnp.sqrt(jnp.sqrt(power)))
    row2 = lax.broadcasted_iota(jnp.int32, (n, 2 * n), 0)
    col2 = lax.broadcasted_iota(jnp.int32, (n, 2 * n), 1)
    shifted = whole(jnp.where(row2 == col2, 1.0, 0.0) - top / shift)
    hi, lo = halves(shifted)
    a_hi[...] = hi
    a_lo[...] = lo
    w_ref[...] = jnp.concatenate([shifted[:NOISE_DIM], shifted[n : n + NOISE_DIM]], axis=0)
    eye = jnp.where(row == col, 1.0, 0.0)

    def step(coefs, apply_a, precise):
        a, b, c = coefs
        basis = w_ref[...]
        parts = halves(basis)
        gram = dot_nt(parts[0], parts[0])
        if precise:
            gram = gram + (dot_nt(parts[0], parts[1]) + dot_nt(parts[1], parts[0]))
            gram_parts = halves(gram)
            gram2 = product_half(gram_parts, gram_parts)
        else:
            low = gram.astype(jnp.bfloat16)
            gram2 = dot(low, low)
        if apply_a:
            moved = halves(product(parts, (a_hi[...], a_lo[...])))
        else:
            moved = parts
        mix = halves(a * eye + b * gram + c * gram2)
        w_ref[...] = product_half(mix, moved)

    @pl.loop(0, ITERS - 1)
    def _(_):
        step(GROW, True, False)

    @pl.loop(0, EXTRA)
    def _(_):
        step(GROW, False, False)

    step(CLOSE[0], False, False)
    step(CLOSE[1], False, False)
    step(CLOSE[2], False, True)
    basis = w_ref[...]
    slope = jnp.pi / beams_total
    bias = -slope * jnp.sum(basis[:, n:], axis=1, keepdims=True)
    lead = halves(basis[:, :n])

    @pl.loop(0, grid_ref.shape[1] // CHUNK)
    def _(i):
        where = pl.ds(pl.multiple_of(i * CHUNK, CHUNK), CHUNK)
        position = (grid_ref[:, where].astype(jnp.float32) + 0.5) / OVERSAMPLE
        offset = position - lax.broadcasted_iota(jnp.int32, (n, CHUNK), 0).astype(jnp.float32)
        angle = (slope * offset) * (slope * offset)
        cot = 1.0 / offset - (slope * slope * offset) * (1.0 / 3.0 + angle * (1.0 / 45.0 + angle * (2.0 / 945.0)))
        projected = product_half(lead, halves(cot)) + bias
        energy = jnp.sum(projected * projected, axis=0, keepdims=True)
        length = jnp.sum(cot * cot, axis=0, keepdims=True) + n * slope * slope
        out_ref[:, where] = 1.0 / (energy / length + spectral_floor)


def finish_user(packed, count, grid_index, beams_total):
    n = WIN_BEAMS
    vmem = pl.BlockSpec(memory_space=pltpu.VMEM)
    return pl.pallas_call(
        functools.partial(finish_kernel, beams_total),
        out_shape=jax.ShapeDtypeStruct(grid_index.shape, jnp.float32),
        in_specs=[vmem, pl.BlockSpec(memory_space=pltpu.SMEM), vmem],
        out_specs=vmem,
        scratch_shapes=[
            pltpu.VMEM((2 * n, 2 * n), jnp.bfloat16),
            pltpu.VMEM((2 * n, 2 * n), jnp.bfloat16),
            pltpu.VMEM((n, 2 * n), jnp.float32),
        ],
        name="finish_user",
    )(packed, count, grid_index)


def local(beam_data, window_count, slot_owner, slot_window, grid_index):
    beam_count = lax.axis_size("beam")
    user_count = window_count.shape[0]
    slot_count = slot_window.shape[1]
    window_width = WIN_BEAMS
    local_windows = beam_data.shape[1] // window_width
    slot_cap = (user_count * slot_count + beam_count - 1) // beam_count + 1
    beams_total = beam_data.shape[1] * beam_count
    snap_local = beam_data.shape[2]
    owners = slot_owner[:, :, 0]
    window_view = beam_data.reshape(2, local_windows, window_width, snap_local)
    same_part, cross_part = local_grams(window_view)
    packed_part = pack_upper(same_part, cross_part - jnp.swapaxes(cross_part, 1, 2))
    window_packed = total_of_pieces(packed_part, "grp")
    requests, flat_slot = owner_slots(
        owners.reshape(-1), slot_window.reshape(-1), beam_count, slot_cap
    )
    picked = jnp.take(
        window_packed,
        lax.all_to_all(requests, "beam", split_axis=0, concat_axis=0, tiled=True),
        axis=0,
    )
    got_packed = lax.all_to_all(picked, "beam", split_axis=0, concat_axis=0, tiled=True)
    picked_packed = jnp.take(
        got_packed.reshape(beam_count * slot_cap, window_width, window_width), flat_slot, axis=0
    )
    picked_packed = picked_packed.reshape(user_count, slot_count, window_width, window_width)
    live = jnp.arange(slot_count, dtype=jnp.int32)[None, :] < window_count[:, None]
    packed = jnp.sum(jnp.where(live[:, :, None, None], picked_packed, 0.0), axis=1)[0]
    return finish_user(packed, window_count, grid_index, beams_total)


def solution(mesh):
    placed = (
        P(None, "beam", "grp"),
        P(("beam", "grp")),
        P(("beam", "grp"), None, None),
        P(("beam", "grp"), None),
        P(("beam", "grp"), None),
    )
    return jax.shard_map(
        local, mesh=mesh, in_specs=placed, out_specs=P(("beam", "grp"), None), check_vma=False
    )
```

```python
import functools

import jax
import jax.numpy as jnp
from jax import lax
from jax.experimental import pallas as pl
from jax.experimental.pallas import tpu as pltpu
from jax.sharding import PartitionSpec as P

WIN_BEAMS = 128
NOISE_DIM = 64
SNAPS = 256
OVERSAMPLE = 32
ITERS = 8
SIDE = 4
MESH = pl.DeviceIdType.MESH

shift_factor = 1.05
spectral_floor = 0.05


def remote(source, target, send_sem, recv_sem, device):
    return pltpu.make_async_remote_copy(
        src_ref=source,
        dst_ref=target,
        send_sem=send_sem,
        recv_sem=recv_sem,
        device_id=device,
        device_id_type=MESH,
    )


def dot_tn(left, right):
    return lax.dot_general(
        left, right, (((0,), (0,)), ((), ())), preferred_element_type=jnp.float32
    )


def exchange_kernel(
    groups, slots, x_ref, meta_ref, out_ref, raw, metas, chosen, blocks, sums, parts,
    raw_send, raw_recv, meta_send, meta_recv, block_send, block_recv, part_send, part_recv, local_sem,
):
    b, g = lax.axis_index("beam"), lax.axis_index("grp")
    core, x, y = b % 2, b // (2 * SIDE), (b // 2) % SIDE
    rows = WIN_BEAMS // 2

    def along(first, second):
        at_x = (x + first * (1 - core) + second * core) % SIDE
        at_y = (y + first * core + second * (1 - core)) % SIDE
        return (at_x * SIDE + at_y) * 2 + core

    partner = b + 1 - 2 * core
    line = [(g + d) % groups for d in range(groups)]
    barrier = pltpu.get_barrier_semaphore()
    greeted = [(b, line[d]) for d in range(1, groups)]
    greeted += [(along(d, 0), g) for d in range(1, SIDE)] + [(along(0, d), g) for d in range(1, SIDE)]
    greeted += [(partner, g)]
    for device in greeted:
        pl.semaphore_signal(barrier, inc=1, device_id=device, device_id_type=MESH)
    pl.semaphore_wait(barrier, len(greeted))

    sent = []

    def send(*args):
        copy = remote(*args)
        copy.start()
        sent.append(copy)

    for d in range(1, groups):
        send(x_ref.at[line[d] // 2], raw.at[g], raw_send.at[d], raw_recv.at[g], (b, line[d]))
    for d in range(1, groups):
        send(meta_ref, metas.at[g], meta_send.at[d], meta_recv.at[g], (b, line[d]))
    raw[g] = x_ref[g // 2]
    metas[g] = meta_ref[...]
    for d in range(1, groups):
        remote(x_ref.at[0], raw.at[line[d]], raw_send.at[d], raw_recv.at[line[d]], (b, line[d])).wait_recv()
    real = raw[:, 0].reshape(SNAPS, WIN_BEAMS)
    imag = raw[:, 1].reshape(SNAPS, WIN_BEAMS)
    same = dot_tn(real, real) + dot_tn(imag, imag)
    cross = dot_tn(imag, real) - dot_tn(real, imag)
    row = lax.broadcasted_iota(jnp.int32, (WIN_BEAMS, WIN_BEAMS), 0)
    col = lax.broadcasted_iota(jnp.int32, (WIN_BEAMS, WIN_BEAMS), 1)
    packed = jnp.where(row <= col, same, cross)
    blocks[b] = jnp.where(g % 2 == 0, packed[:rows], packed[rows:])

    count = [0]

    def pass_on(block, device):
        send(blocks.at[block], blocks.at[block], block_send.at[count[0]], block_recv.at[block], (device, g))
        count[0] += 1

    def arrived(block):
        remote(blocks.at[block], blocks.at[block], block_send.at[0], block_recv.at[block], (partner, g)).wait_recv()

    for d in (1, 3, 2):
        pass_on(b, along(d, 0))
    for d in (1, 3, 2):
        pass_on(b, along(0, d))
    pass_on(b, partner)
    for d in range(1, groups):
        remote(meta_ref, metas.at[line[d]], meta_send.at[d], meta_recv.at[line[d]], (b, line[d])).wait_recv()
    fetch = pltpu.make_async_copy(metas, chosen, local_sem)
    fetch.start()
    for e in (1, 3, 2):
        block = along(e, 0)
        arrived(block)
        for d in (1, 3, 2):
            pass_on(block, along(0, d))
        pass_on(block, partner)
    for e in (0, 1, 3, 2):
        for d in (1, 3, 2):
            block = along(e, d)
            arrived(block)
            pass_on(block, partner)
    fetch.wait()
    for i in range(SIDE * SIDE):
        arrived(2 * i + 1 - core)

    for d in list(range(1, groups)) + [0]:
        user = line[d]
        total = jnp.zeros((rows, WIN_BEAMS), jnp.float32)
        for k in range(slots):
            weight = jnp.where(chosen[user, 0, slots + k] == g // 2, 1.0, 0.0)
            total = total + weight * blocks[chosen[user, 0, k]]
        if d == 0:
            parts[g] = total
        else:
            sums[d] = total
            send(sums.at[d], parts.at[g], part_send.at[d], part_recv.at[g], (b, user))
    for d in range(1, groups):
        remote(sums.at[d], parts.at[line[d]], part_send.at[d], part_recv.at[line[d]], (b, line[d])).wait_recv()
    for h in range(2):
        total = parts[h]
        for w in range(1, groups // 2):
            total = total + parts[2 * w + h]
        out_ref[h * rows : (h + 1) * rows, :] = total
    for copy in sent:
        copy.wait_send()


def exchange(x, meta, groups, owners, slots):
    rows = WIN_BEAMS // 2
    vmem = pl.BlockSpec(memory_space=pltpu.VMEM)
    dma = pltpu.SemaphoreType.DMA
    forwards = 2 * (SIDE - 1) + 1 + (SIDE - 1) * SIDE + SIDE * (SIDE - 1)
    return pl.pallas_call(
        functools.partial(exchange_kernel, groups, slots),
        out_shape=jax.ShapeDtypeStruct((WIN_BEAMS, WIN_BEAMS), jnp.float32),
        in_specs=[vmem, vmem],
        out_specs=vmem,
        scratch_shapes=[
            pltpu.VMEM((groups,) + x.shape[1:], x.dtype),
            pltpu.VMEM((groups,) + meta.shape, meta.dtype),
            pltpu.SMEM((groups,) + meta.shape, meta.dtype),
            pltpu.VMEM((owners, rows, WIN_BEAMS), jnp.float32),
            pltpu.VMEM((groups, rows, WIN_BEAMS), jnp.float32),
            pltpu.VMEM((groups, rows, WIN_BEAMS), jnp.float32),
            dma((groups,)),
            dma((groups,)),
            dma((groups,)),
            dma((groups,)),
            dma((forwards,)),
            dma((owners,)),
            dma((groups,)),
            dma((groups,)),
            dma,
        ],
        compiler_params=pltpu.CompilerParams(collective_id=0, has_side_effects=True),
        name="exchange",
    )(x, meta)


GROW = (3.4445, -4.7750, 2.0315)
CLOSE = ((3.109266, -3.792034, 1.535381), (1.90467, -1.282586, 0.3782733), (1.875, -1.25, 0.375))
EXTRA = 6
CHUNK = 512


def halves(value):
    high = value.astype(jnp.bfloat16)
    return high, (value - high.astype(jnp.float32)).astype(jnp.bfloat16)


def dot(left, right):
    return jnp.dot(left, right, preferred_element_type=jnp.float32)


def dot_nt(left, right):
    return lax.dot_general(
        left, right, (((1,), (1,)), ((), ())), preferred_element_type=jnp.float32
    )


def product(left, right):
    return dot(left[0], right[0]) + (dot(left[0], right[1]) + dot(left[1], right[0]))


def product_half(left, right):
    both = dot(
        jnp.concatenate([left[0], left[1]], axis=1),
        jnp.concatenate([right[0], right[0]], axis=0),
    )
    return both + dot(left[0], right[1])


def whole(top):
    n = WIN_BEAMS
    return jnp.concatenate([top, jnp.concatenate([-top[:, n:], top[:, :n]], axis=1)], axis=0)


def finish_kernel(beams_total, packed_ref, count_ref, grid_ref, out_ref, a_hi, a_lo, w_ref):
    n = WIN_BEAMS
    row = lax.broadcasted_iota(jnp.int32, (n, n), 0)
    col = lax.broadcasted_iota(jnp.int32, (n, n), 1)
    packed = packed_ref[...]
    flipped = packed.T
    same = jnp.where(row <= col, packed, flipped)
    imag = jnp.where(row > col, packed, jnp.where(row < col, -flipped, 0.0))
    scale = jnp.full((1, 1), 1.0, jnp.float32) / (count_ref[0].astype(jnp.float32) * SNAPS)
    top = jnp.concatenate([same, -imag], axis=1) * scale
    square = product(halves(top), halves(whole(top)))
    fourth = product(halves(square), halves(whole(square)))
    power = 2.0 * jnp.sum(fourth * fourth, axis=(0, 1), keepdims=True)
    shift = shift_factor * jnp.sqrt(jnp.sqrt(jnp.sqrt(power)))
    row2 = lax.broadcasted_iota(jnp.int32, (n, 2 * n), 0)
    col2 = lax.broadcasted_iota(jnp.int32, (n, 2 * n), 1)
    shifted = whole(jnp.where(row2 == col2, 1.0, 0.0) - top / shift)
    hi, lo = halves(shifted)
    a_hi[...] = hi
    a_lo[...] = lo
    w_ref[...] = jnp.concatenate([shifted[:NOISE_DIM], shifted[n : n + NOISE_DIM]], axis=0)
    eye = jnp.where(row == col, 1.0, 0.0)

    def step(coefs, apply_a, precise):
        a, b, c = coefs
        basis = w_ref[...]
        parts = halves(basis)
        gram = dot_nt(parts[0], parts[0])
        if precise:
            gram = gram + (dot_nt(parts[0], parts[1]) + dot_nt(parts[1], parts[0]))
            gram_parts = halves(gram)
            gram2 = product_half(gram_parts, gram_parts)
        else:
            low = gram.astype(jnp.bfloat16)
            gram2 = dot(low, low)
        if apply_a:
            moved = halves(product(parts, (a_hi[...], a_lo[...])))
        else:
            moved = parts
        mix = halves(a * eye + b * gram + c * gram2)
        w_ref[...] = product_half(mix, moved)

    @pl.loop(0, ITERS - 1)
    def _(_):
        step(GROW, True, False)

    @pl.loop(0, EXTRA)
    def _(_):
        step(GROW, False, False)

    step(CLOSE[0], False, False)
    step(CLOSE[1], False, False)
    step(CLOSE[2], False, True)
    basis = w_ref[...]
    slope = jnp.pi / beams_total
    bias = -slope * jnp.sum(basis[:, n:], axis=1, keepdims=True)
    lead = halves(basis[:, :n])

    @pl.loop(0, grid_ref.shape[1] // CHUNK)
    def _(i):
        where = pl.ds(pl.multiple_of(i * CHUNK, CHUNK), CHUNK)
        position = (grid_ref[:, where].astype(jnp.float32) + 0.5) / OVERSAMPLE
        offset = position - lax.broadcasted_iota(jnp.int32, (n, CHUNK), 0).astype(jnp.float32)
        angle = (slope * offset) * (slope * offset)
        cot = 1.0 / offset - (slope * slope * offset) * (1.0 / 3.0 + angle * (1.0 / 45.0 + angle * (2.0 / 945.0)))
        projected = product_half(lead, halves(cot)) + bias
        energy = jnp.sum(projected * projected, axis=0, keepdims=True)
        length = jnp.sum(cot * cot, axis=0, keepdims=True) + n * slope * slope
        out_ref[:, where] = 1.0 / (energy / length + spectral_floor)


def finish_user(packed, count, grid_index, beams_total):
    n = WIN_BEAMS
    vmem = pl.BlockSpec(memory_space=pltpu.VMEM)
    return pl.pallas_call(
        functools.partial(finish_kernel, beams_total),
        out_shape=jax.ShapeDtypeStruct(grid_index.shape, jnp.float32),
        in_specs=[vmem, pl.BlockSpec(memory_space=pltpu.SMEM), vmem],
        out_specs=vmem,
        scratch_shapes=[
            pltpu.VMEM((2 * n, 2 * n), jnp.bfloat16),
            pltpu.VMEM((2 * n, 2 * n), jnp.bfloat16),
            pltpu.VMEM((n, 2 * n), jnp.float32),
        ],
        name="finish_user",
    )(packed, count, grid_index)


def local(beam_data, window_count, slot_owner, slot_window, grid_index):
    owners, groups = lax.axis_size("beam"), lax.axis_size("grp")
    slots = slot_window.shape[1]
    windows = beam_data.shape[1] // WIN_BEAMS
    x = beam_data.reshape(2, windows, WIN_BEAMS, beam_data.shape[2]).transpose(1, 0, 3, 2)
    live = jnp.arange(slots, dtype=jnp.int32)[None, :] < window_count[:, None]
    words = jnp.concatenate([slot_owner[:, :, 0], jnp.where(live, slot_window, -1)], axis=1)
    meta = jnp.broadcast_to(jnp.pad(words, ((0, 0), (0, 128 - 2 * slots))), (8, 128))
    packed = exchange(x, meta, groups, owners, slots)
    return finish_user(packed, window_count, grid_index, beam_data.shape[1] * owners)


def solution(mesh):
    placed = (
        P(None, "beam", "grp"),
        P(("beam", "grp")),
        P(("beam", "grp"), None, None),
        P(("beam", "grp"), None),
        P(("beam", "grp"), None),
    )
    return jax.shard_map(
        local, mesh=mesh, in_specs=placed, out_specs=P(("beam", "grp"), None), check_vma=False
    )
```

```python
import functools

import jax
import jax.numpy as jnp
from jax import lax
from jax.experimental import pallas as pl
from jax.experimental.pallas import tpu as pltpu
from jax.sharding import PartitionSpec as P

WIN_BEAMS = 128
NOISE_DIM = 64
SNAPS = 256
OVERSAMPLE = 32
ITERS = 8
SIDE = 4
MESH = pl.DeviceIdType.MESH

shift_factor = 1.05
spectral_floor = 0.05


def remote(source, target, send_sem, recv_sem, device):
    return pltpu.make_async_remote_copy(
        src_ref=source,
        dst_ref=target,
        send_sem=send_sem,
        recv_sem=recv_sem,
        device_id=device,
        device_id_type=MESH,
    )


def dot_tn(left, right):
    return lax.dot_general(
        left, right, (((0,), (0,)), ((), ())), preferred_element_type=jnp.float32
    )


def exchange_kernel(
    groups, slots, x_ref, count_ref, owner_ref, window_ref, out_ref, meta_ref, raw, metas, chosen, blocks, sums, parts,
    raw_send, raw_recv, meta_send, meta_recv, block_send, block_recv, part_send, part_recv, local_sem,
):
    b, g = lax.axis_index("beam"), lax.axis_index("grp")
    core, x, y = b % 2, b // (2 * SIDE), (b // 2) % SIDE
    rows = WIN_BEAMS // 2

    def along(first, second):
        at_x = (x + first * (1 - core) + second * core) % SIDE
        at_y = (y + first * core + second * (1 - core)) % SIDE
        return (at_x * SIDE + at_y) * 2 + core

    def window_of(w):
        return x_ref.at[:, :, pl.ds(pl.multiple_of(w * WIN_BEAMS, WIN_BEAMS), WIN_BEAMS)]

    partner = b + 1 - 2 * core
    line = [(g + d) % groups for d in range(groups)]
    barrier = pltpu.get_barrier_semaphore()
    greeted = [(b, line[d]) for d in range(1, groups)]
    greeted += [(along(d, 0), g) for d in range(1, SIDE)] + [(along(0, d), g) for d in range(1, SIDE)]
    greeted += [(partner, g)]
    lane = lax.broadcasted_iota(jnp.int32, meta_ref.shape, 1)
    meta = jnp.full(meta_ref.shape, -1, jnp.int32)
    for k in range(slots):
        wanted = jnp.where(k < count_ref[0], window_ref[0, k], -1)
        meta = jnp.where(lane == k, owner_ref[0, k], jnp.where(lane == slots + k, wanted, meta))
    meta_ref[...] = meta
    for device in greeted:
        pl.semaphore_signal(barrier, inc=1, device_id=device, device_id_type=MESH)
    pl.semaphore_wait(barrier, len(greeted))

    sent = []

    def send(*args):
        copy = remote(*args)
        copy.start()
        sent.append(copy)

    for d in range(1, groups):
        send(window_of(line[d] // 2), raw.at[g], raw_send.at[d], raw_recv.at[g], (b, line[d]))
    for d in range(1, groups):
        send(meta_ref, metas.at[g], meta_send.at[d], meta_recv.at[g], (b, line[d]))
    raw[g] = window_of(g // 2)[...]
    metas[g] = meta_ref[...]
    for d in range(1, groups):
        remote(window_of(0), raw.at[line[d]], raw_send.at[d], raw_recv.at[line[d]], (b, line[d])).wait_recv()
    real = raw[:, 0].reshape(SNAPS, WIN_BEAMS)
    imag = raw[:, 1].reshape(SNAPS, WIN_BEAMS)
    same = dot_tn(real, real) + dot_tn(imag, imag)
    cross = dot_tn(imag, real) - dot_tn(real, imag)
    row = lax.broadcasted_iota(jnp.int32, (WIN_BEAMS, WIN_BEAMS), 0)
    col = lax.broadcasted_iota(jnp.int32, (WIN_BEAMS, WIN_BEAMS), 1)
    packed = jnp.where(row <= col, same, cross)
    blocks[b] = jnp.where(g % 2 == 0, packed[:rows], packed[rows:])

    count = [0]

    def pass_on(block, device):
        send(blocks.at[block], blocks.at[block], block_send.at[count[0]], block_recv.at[block], (device, g))
        count[0] += 1

    def arrived(block):
        remote(blocks.at[block], blocks.at[block], block_send.at[0], block_recv.at[block], (partner, g)).wait_recv()

    for d in (1, 3, 2):
        pass_on(b, along(d, 0))
    for d in (1, 3, 2):
        pass_on(b, along(0, d))
    pass_on(b, partner)
    for d in range(1, groups):
        remote(meta_ref, metas.at[line[d]], meta_send.at[d], meta_recv.at[line[d]], (b, line[d])).wait_recv()
    fetch = pltpu.make_async_copy(metas, chosen, local_sem)
    fetch.start()
    for e in (1, 3, 2):
        block = along(e, 0)
        arrived(block)
        for d in (1, 3, 2):
            pass_on(block, along(0, d))
        pass_on(block, partner)
    for e in (0, 1, 3, 2):
        for d in (1, 3, 2):
            block = along(e, d)
            arrived(block)
            pass_on(block, partner)
    fetch.wait()
    for i in range(SIDE * SIDE):
        arrived(2 * i + 1 - core)

    for d in list(range(1, groups)) + [0]:
        user = line[d]
        total = jnp.zeros((rows, WIN_BEAMS), jnp.float32)
        for k in range(slots):
            weight = jnp.where(chosen[user, 0, slots + k] == g // 2, 1.0, 0.0)
            total = total + weight * blocks[chosen[user, 0, k]]
        if d == 0:
            parts[g] = total
        else:
            sums[d] = total
            send(sums.at[d], parts.at[g], part_send.at[d], part_recv.at[g], (b, user))
    for d in range(1, groups):
        remote(sums.at[d], parts.at[line[d]], part_send.at[d], part_recv.at[line[d]], (b, line[d])).wait_recv()
    for h in range(2):
        total = parts[h]
        for w in range(1, groups // 2):
            total = total + parts[2 * w + h]
        out_ref[h * rows : (h + 1) * rows, :] = total
    for copy in sent:
        copy.wait_send()


def exchange(x, count, owner, window, groups, owners, slots):
    rows = WIN_BEAMS // 2
    vmem, smem = pl.BlockSpec(memory_space=pltpu.VMEM), pl.BlockSpec(memory_space=pltpu.SMEM)
    meta = (8, 128)
    dma = pltpu.SemaphoreType.DMA
    forwards = 2 * (SIDE - 1) + 1 + (SIDE - 1) * SIDE + SIDE * (SIDE - 1)
    return pl.pallas_call(
        functools.partial(exchange_kernel, groups, slots),
        out_shape=jax.ShapeDtypeStruct((WIN_BEAMS, WIN_BEAMS), jnp.float32),
        in_specs=[vmem, smem, smem, smem],
        out_specs=vmem,
        scratch_shapes=[
            pltpu.VMEM(meta, jnp.int32),
            pltpu.VMEM((groups,) + x.shape[:2] + (WIN_BEAMS,), x.dtype),
            pltpu.VMEM((groups,) + meta, jnp.int32),
            pltpu.SMEM((groups,) + meta, jnp.int32),
            pltpu.VMEM((owners, rows, WIN_BEAMS), jnp.float32),
            pltpu.VMEM((groups, rows, WIN_BEAMS), jnp.float32),
            pltpu.VMEM((groups, rows, WIN_BEAMS), jnp.float32),
            dma((groups,)),
            dma((groups,)),
            dma((groups,)),
            dma((groups,)),
            dma((forwards,)),
            dma((owners,)),
            dma((groups,)),
            dma((groups,)),
            dma,
        ],
        compiler_params=pltpu.CompilerParams(collective_id=0, has_side_effects=True),
        name="exchange",
    )(x, count, owner, window)


GROW = (3.4445, -4.7750, 2.0315)
CLOSE = ((3.109266, -3.792034, 1.535381), (1.90467, -1.282586, 0.3782733))
LAST = (1.875, -1.25, 0.375)
NEAR = 0.012
ROUNDS = 8
PIECES = 8


def halves(value):
    high = value.astype(jnp.bfloat16)
    return high, (value - high.astype(jnp.float32)).astype(jnp.bfloat16)


def dot(left, right):
    return jnp.dot(left, right, preferred_element_type=jnp.float32)


def dot_nt(left, right):
    return lax.dot_general(
        left, right, (((1,), (1,)), ((), ())), preferred_element_type=jnp.float32
    )


def product(left, right):
    return dot(left[0], right[0]) + (dot(left[0], right[1]) + dot(left[1], right[0]))


def product_half(left, right):
    both = dot(
        jnp.concatenate([left[0], left[1]], axis=1),
        jnp.concatenate([right[0], right[0]], axis=0),
    )
    return both + dot(left[0], right[1])


def whole(top):
    n = WIN_BEAMS
    return jnp.concatenate([top, jnp.concatenate([-top[:, n:], top[:, :n]], axis=1)], axis=0)


def finish_kernel(
    beams_total, packed_ref, count_ref, grid_ref, out_ref, a_hi, a_lo, w_ref, gram_ref, c_hi, c_lo, length_ref
):
    n = WIN_BEAMS
    chunk = grid_ref.shape[1] // PIECES
    slope = jnp.pi / beams_total
    row = lax.broadcasted_iota(jnp.int32, (n, n), 0)
    col = lax.broadcasted_iota(jnp.int32, (n, n), 1)
    packed = packed_ref[...]
    flipped = packed.T
    same = jnp.where(row <= col, packed, flipped)
    imag = jnp.where(row > col, packed, jnp.where(row < col, -flipped, 0.0))
    scale = jnp.full((1, 1), 1.0, jnp.float32) / (count_ref[0].astype(jnp.float32) * SNAPS)
    top = jnp.concatenate([same, -imag], axis=1) * scale
    square = product(halves(top), halves(whole(top)))
    fourth = product(halves(square), halves(whole(square)))
    power = 2.0 * jnp.sum(fourth * fourth, axis=(0, 1), keepdims=True)
    shift = shift_factor * jnp.sqrt(jnp.sqrt(jnp.sqrt(power)))
    row2 = lax.broadcasted_iota(jnp.int32, (n, 2 * n), 0)
    col2 = lax.broadcasted_iota(jnp.int32, (n, 2 * n), 1)
    shifted = whole(jnp.where(row2 == col2, 1.0, 0.0) - top / shift)
    hi, lo = halves(shifted)
    a_hi[...] = hi
    a_lo[...] = lo
    w_ref[...] = jnp.concatenate([shifted[:NOISE_DIM], shifted[n : n + NOISE_DIM]], axis=0)
    eye = jnp.where(row == col, 1.0, 0.0)

    def steer(piece):
        where = pl.ds(pl.multiple_of(piece * chunk, chunk), chunk)
        position = (grid_ref[:, where].astype(jnp.float32) + 0.5) / OVERSAMPLE
        offset = position - lax.broadcasted_iota(jnp.int32, (n, chunk), 0).astype(jnp.float32)
        angle = (slope * offset) * (slope * offset)
        series = 1.0 / 3.0 + angle * (1.0 / 45.0 + angle * (2.0 / 945.0))
        cot = 1.0 / offset - (slope * slope * offset) * series
        high, low = halves(cot)
        c_hi[:, where] = high
        c_lo[:, where] = low
        length_ref[:, where] = jnp.sum(cot * cot, axis=0, keepdims=True) + n * slope * slope

    def step(coefs, apply_a=False):
        a, b, c = coefs
        parts = halves(w_ref[...])
        gram = dot_nt(parts[0], parts[0])
        low = gram.astype(jnp.bfloat16)
        mix = a * eye + b * gram + c * dot(low, low)
        moved = halves(product(parts, (a_hi[...], a_lo[...]))) if apply_a else parts
        w_ref[...] = product_half(halves(mix), moved)

    def distance():
        parts = halves(w_ref[...])
        cross = dot_nt(parts[0], parts[1])
        gram = dot_nt(parts[0], parts[0]) + (cross + dot_nt(parts[1], parts[0]))
        gram_ref[...] = gram
        return jnp.sum((gram - eye) * (gram - eye))

    @pl.loop(0, ITERS - 1)
    def _(i):
        step(GROW, True)
        steer(i)

    step(CLOSE[0])
    steer(ITERS - 1)
    step(CLOSE[1])

    def again(state):
        step(GROW)
        step(GROW)
        step(CLOSE[0])
        step(CLOSE[1])
        return state[0] + 1, distance()

    lax.while_loop(
        lambda state: (state[1] > NEAR) & (state[0] < ROUNDS), again, (jnp.int32(0), distance())
    )
    gram = gram_ref[...]
    parts = halves(gram)
    mix = LAST[0] * eye + LAST[1] * gram + LAST[2] * product_half(parts, parts)
    basis = product_half(halves(mix), halves(w_ref[...]))
    bias = -slope * jnp.sum(basis[:, n:], axis=1, keepdims=True)
    lead = halves(basis[:, :n])
    for piece in range(PIECES):
        where = slice(piece * chunk, (piece + 1) * chunk)
        projected = product_half(lead, (c_hi[:, where], c_lo[:, where])) + bias
        energy = jnp.sum(projected * projected, axis=0, keepdims=True)
        out_ref[:, where] = 1.0 / (energy / length_ref[:, where] + spectral_floor)


def finish_user(packed, count, grid_index, beams_total):
    n = WIN_BEAMS
    points = grid_index.shape[1]
    vmem = pl.BlockSpec(memory_space=pltpu.VMEM)
    return pl.pallas_call(
        functools.partial(finish_kernel, beams_total),
        out_shape=jax.ShapeDtypeStruct(grid_index.shape, jnp.float32),
        in_specs=[vmem, pl.BlockSpec(memory_space=pltpu.SMEM), vmem],
        out_specs=vmem,
        scratch_shapes=[
            pltpu.VMEM((2 * n, 2 * n), jnp.bfloat16),
            pltpu.VMEM((2 * n, 2 * n), jnp.bfloat16),
            pltpu.VMEM((n, 2 * n), jnp.float32),
            pltpu.VMEM((n, n), jnp.float32),
            pltpu.VMEM((n, points), jnp.bfloat16),
            pltpu.VMEM((n, points), jnp.bfloat16),
            pltpu.VMEM((1, points), jnp.float32),
        ],
        name="finish_user",
    )(packed, count, grid_index)


def local(beam_data, window_count, slot_owner, slot_window, grid_index):
    owners, groups = lax.axis_size("beam"), lax.axis_size("grp")
    slots = slot_window.shape[1]
    x = beam_data.transpose(0, 2, 1)
    packed = exchange(x, window_count, slot_owner[:, :, 0], slot_window, groups, owners, slots)
    return finish_user(packed, window_count, grid_index, beam_data.shape[1] * owners)


def solution(mesh):
    placed = (
        P(None, "beam", "grp"),
        P(("beam", "grp")),
        P(("beam", "grp"), None, None),
        P(("beam", "grp"), None),
        P(("beam", "grp"), None),
    )
    return jax.shard_map(
        local, mesh=mesh, in_specs=placed, out_specs=P(("beam", "grp"), None), check_vma=False
    )
```

```python
import functools

import jax
import jax.numpy as jnp
from jax import lax
from jax.experimental import pallas as pl
from jax.experimental.pallas import tpu as pltpu
from jax.sharding import PartitionSpec as P

WIN_BEAMS = 128
NOISE_DIM = 64
SNAPS = 256
OVERSAMPLE = 32
ITERS = 8
SIDE = 4
MESH = pl.DeviceIdType.MESH

shift_factor = 1.05
spectral_floor = 0.05


def remote(source, target, send_sem, recv_sem, device):
    return pltpu.make_async_remote_copy(
        src_ref=source,
        dst_ref=target,
        send_sem=send_sem,
        recv_sem=recv_sem,
        device_id=device,
        device_id_type=MESH,
    )


def dot_tn(left, right):
    return lax.dot_general(
        left, right, (((0,), (0,)), ((), ())), preferred_element_type=jnp.float32
    )


def exchange_kernel(
    groups, slots, x_ref, count_ref, owner_ref, window_ref, out_ref, meta_ref, partial, pieces, metas, chosen, blocks,
    ready, sums, piece_send, piece_recv, meta_send, meta_recv, block_send, block_recv, sum_send, sum_recv, local_sem,
):
    b, g = lax.axis_index("beam"), lax.axis_index("grp")
    core, x, y = b % 2, b // (2 * SIDE), (b // 2) % SIDE
    windows, rows = blocks.shape[1:3]

    def along(first, second):
        at_x = (x + first * (1 - core) + second * core) % SIDE
        at_y = (y + first * core + second * (1 - core)) % SIDE
        return (at_x * SIDE + at_y) * 2 + core

    partner = b + 1 - 2 * core
    line = [(g + d) % groups for d in range(groups)]
    order = sorted(range(1, groups), key=lambda d: -min(d, groups - d))
    barrier = pltpu.get_barrier_semaphore()
    greeted = [(b, line[d]) for d in order]
    greeted += [(along(d, 0), g) for d in range(1, SIDE)] + [(along(0, d), g) for d in range(1, SIDE)]
    greeted += [(partner, g)]
    for device in greeted:
        pl.semaphore_signal(barrier, inc=1, device_id=device, device_id_type=MESH)

    lane = lax.broadcasted_iota(jnp.int32, meta_ref.shape, 1)
    meta = jnp.full(meta_ref.shape, -1, jnp.int32)
    for k in range(slots):
        wanted = jnp.where(k < count_ref[0], window_ref[0, k], -1)
        meta = jnp.where(lane == k, owner_ref[0, k], jnp.where(lane == slots + k, wanted, meta))
    meta_ref[...] = meta
    row = lax.broadcasted_iota(jnp.int32, (WIN_BEAMS, WIN_BEAMS), 0)
    col = lax.broadcasted_iota(jnp.int32, (WIN_BEAMS, WIN_BEAMS), 1)
    for w in range(windows):
        real = x_ref[0, :, w * WIN_BEAMS : (w + 1) * WIN_BEAMS]
        imag = x_ref[1, :, w * WIN_BEAMS : (w + 1) * WIN_BEAMS]
        same = dot_tn(real, real) + dot_tn(imag, imag)
        cross = dot_tn(imag, real) - dot_tn(real, imag)
        packed = jnp.where(row <= col, same, cross)
        for s in range(groups):
            partial[s, w] = packed[s * rows : (s + 1) * rows]
    pl.semaphore_wait(barrier, len(greeted))

    sent = []

    def send(*args):
        copy = remote(*args)
        copy.start()
        sent.append(copy)

    for d in order:
        send(partial.at[line[d]], pieces.at[g], piece_send.at[d], piece_recv.at[g], (b, line[d]))
    for d in order:
        send(meta_ref, metas.at[g], meta_send.at[d], meta_recv.at[g], (b, line[d]))
    metas[g] = meta_ref[...]
    own = partial[g]
    for d in reversed(order):
        piece = pieces.at[line[d]]
        remote(piece, piece, piece_send.at[d], piece_recv.at[line[d]], (b, line[d])).wait_recv()
        own = own + pieces[line[d]]
    blocks[b] = own

    count = [0]

    def pass_on(block, device):
        piece = blocks.at[block]
        send(piece, piece, block_send.at[count[0]], block_recv.at[block], (device, g))
        count[0] += 1

    def arrived(block):
        piece = blocks.at[block]
        remote(piece, piece, block_send.at[0], block_recv.at[block], (partner, g)).wait_recv()

    for d in (2, 1, 3):
        pass_on(b, along(d, 0))
    for d in (2, 1, 3):
        pass_on(b, along(0, d))
    pass_on(b, partner)
    for d in range(1, groups):
        remote(meta_ref, metas.at[line[d]], meta_send.at[d], meta_recv.at[line[d]], (b, line[d])).wait_recv()
    fetch = pltpu.make_async_copy(metas, chosen, local_sem)
    fetch.start()
    for e in (1, 3, 2):
        block = along(e, 0)
        arrived(block)
        for d in (2, 1, 3):
            pass_on(block, along(0, d))
        pass_on(block, partner)
    for e in (0, 1, 3, 2):
        for d in (1, 3, 2):
            block = along(e, d)
            arrived(block)
            pass_on(block, partner)
    fetch.wait()
    for i in range(SIDE * SIDE):
        arrived(2 * i + 1 - core)

    for d in order + [0]:
        total = jnp.zeros((rows, WIN_BEAMS), jnp.float32)
        for k in range(slots):
            wanted = chosen[line[d], 0, slots + k]
            weight = jnp.where(wanted >= 0, 1.0, 0.0)
            total = total + weight * blocks[chosen[line[d], 0, k], jnp.maximum(wanted, 0)]
        if d == 0:
            out_ref[g] = total
        else:
            ready[d] = total
            send(ready.at[d], sums.at[g], sum_send.at[d], sum_recv.at[g], (b, line[d]))
    for d in range(1, groups):
        piece = sums.at[line[d]]
        remote(piece, piece, sum_send.at[d], sum_recv.at[line[d]], (b, line[d])).wait_recv()
        out_ref[line[d]] = sums[line[d]]
    for copy in sent:
        copy.wait_send()


def exchange(x, count, owner, window, groups, owners, slots):
    windows, rows = x.shape[2] // WIN_BEAMS, WIN_BEAMS // groups
    vmem, smem = pl.BlockSpec(memory_space=pltpu.VMEM), pl.BlockSpec(memory_space=pltpu.SMEM)
    meta = (8, 128)
    dma = pltpu.SemaphoreType.DMA
    forwards = 2 * (SIDE - 1) + 1 + (SIDE - 1) * SIDE + SIDE * (SIDE - 1)
    return pl.pallas_call(
        functools.partial(exchange_kernel, groups, slots),
        out_shape=jax.ShapeDtypeStruct((groups, rows, WIN_BEAMS), jnp.float32),
        in_specs=[vmem, smem, smem, smem],
        out_specs=vmem,
        scratch_shapes=[
            pltpu.VMEM(meta, jnp.int32),
            pltpu.VMEM((groups, windows, rows, WIN_BEAMS), jnp.float32),
            pltpu.VMEM((groups, windows, rows, WIN_BEAMS), jnp.float32),
            pltpu.VMEM((groups,) + meta, jnp.int32),
            pltpu.SMEM((groups,) + meta, jnp.int32),
            pltpu.VMEM((owners, windows, rows, WIN_BEAMS), jnp.float32),
            pltpu.VMEM((groups, rows, WIN_BEAMS), jnp.float32),
            pltpu.VMEM((groups, rows, WIN_BEAMS), jnp.float32),
            dma((groups,)),
            dma((groups,)),
            dma((groups,)),
            dma((groups,)),
            dma((forwards,)),
            dma((owners,)),
            dma((groups,)),
            dma((groups,)),
            dma,
        ],
        compiler_params=pltpu.CompilerParams(collective_id=0, has_side_effects=True),
        name="exchange",
    )(x, count, owner, window).reshape(WIN_BEAMS, WIN_BEAMS)


FAST = (2.4, -1.45, 0.0)
GROW = (3.4445, -4.7750, 2.0315)
CLOSE = ((3.109266, -3.792034, 1.535381), (1.90467, -1.282586, 0.3782733))
LAST = (1.875, -1.25, 0.375)
NEAR = 0.016
PIECES = 8


def halves(value):
    high = value.astype(jnp.bfloat16)
    return high, (value - high.astype(jnp.float32)).astype(jnp.bfloat16)


def dot(left, right):
    return jnp.dot(left, right, preferred_element_type=jnp.float32)


def dot_nt(left, right):
    return lax.dot_general(
        left, right, (((1,), (1,)), ((), ())), preferred_element_type=jnp.float32
    )


def product(left, right):
    return dot(left[0], right[0]) + (dot(left[0], right[1]) + dot(left[1], right[0]))


def product_half(left, right):
    both = dot(
        jnp.concatenate([left[0], left[1]], axis=1),
        jnp.concatenate([right[0], right[0]], axis=0),
    )
    return both + dot(left[0], right[1])


def whole(top):
    n = WIN_BEAMS
    return jnp.concatenate([top, jnp.concatenate([-top[:, n:], top[:, :n]], axis=1)], axis=0)


def finish_kernel(
    beams_total, packed_ref, count_ref, grid_ref, out_ref, a_hi, a_lo, start_ref, w_ref, gram_ref, c_hi, c_lo, length_ref
):
    n = WIN_BEAMS
    chunk = grid_ref.shape[1] // PIECES
    slope = jnp.pi / beams_total
    row = lax.broadcasted_iota(jnp.int32, (n, n), 0)
    col = lax.broadcasted_iota(jnp.int32, (n, n), 1)
    packed = packed_ref[...]
    flipped = packed.T
    same = jnp.where(row <= col, packed, flipped)
    imag = jnp.where(row > col, packed, jnp.where(row < col, -flipped, 0.0))
    scale = jnp.full((1, 1), 1.0, jnp.float32) / (count_ref[0].astype(jnp.float32) * SNAPS)
    top = jnp.concatenate([same, -imag], axis=1) * scale
    square = product(halves(top), halves(whole(top)))
    fourth = product(halves(square), halves(whole(square)))
    power = 2.0 * jnp.sum(fourth * fourth, axis=(0, 1), keepdims=True)
    shift = shift_factor * jnp.sqrt(jnp.sqrt(jnp.sqrt(power)))
    row2 = lax.broadcasted_iota(jnp.int32, (n, 2 * n), 0)
    col2 = lax.broadcasted_iota(jnp.int32, (n, 2 * n), 1)
    shifted = whole(jnp.where(row2 == col2, 1.0, 0.0) - top / shift)
    hi, lo = halves(shifted)
    a_hi[...] = hi
    a_lo[...] = lo
    start_ref[...] = jnp.concatenate([shifted[:NOISE_DIM], shifted[n : n + NOISE_DIM]], axis=0)
    w_ref[...] = start_ref[...]
    eye = jnp.where(row == col, 1.0, 0.0)

    def steer(piece):
        where = pl.ds(pl.multiple_of(piece * chunk, chunk), chunk)
        position = (grid_ref[:, where].astype(jnp.float32) + 0.5) / OVERSAMPLE
        offset = position - lax.broadcasted_iota(jnp.int32, (n, chunk), 0).astype(jnp.float32)
        angle = (slope * offset) * (slope * offset)
        series = 1.0 / 3.0 + angle * (1.0 / 45.0 + angle * (2.0 / 945.0))
        cot = 1.0 / offset - (slope * slope * offset) * series
        high, low = halves(cot)
        c_hi[:, where] = high
        c_lo[:, where] = low
        length_ref[:, where] = jnp.sum(cot * cot, axis=0, keepdims=True) + n * slope * slope

    def step(coefs, apply_a=False):
        a, b, c = coefs
        parts = halves(w_ref[...])
        gram = dot_nt(parts[0], parts[0])
        mix = a * eye + b * gram
        if c:
            low = gram.astype(jnp.bfloat16)
            mix = mix + c * dot(low, low)
        moved = halves(product(parts, (a_hi[...], a_lo[...]))) if apply_a else parts
        w_ref[...] = product_half(halves(mix), moved)

    def distance():
        parts = halves(w_ref[...])
        cross = dot_nt(parts[0], parts[1])
        gram = dot_nt(parts[0], parts[0]) + (cross + dot_nt(parts[1], parts[0]))
        gram_ref[...] = gram
        return jnp.sum((gram - eye) * (gram - eye))

    @pl.loop(0, ITERS - 1)
    def _(i):
        step(FAST, True)
        steer(i)

    step(CLOSE[0])
    steer(ITERS - 1)
    step(CLOSE[1])
    off = distance()

    @pl.when(jnp.logical_not(off < NEAR))
    def _():
        w_ref[...] = start_ref[...]

        @pl.loop(0, ITERS - 1)
        def _(_):
            step(GROW)
            step(CLOSE[0])
            step(CLOSE[1], True)

        step(GROW)
        step(CLOSE[0])
        step(CLOSE[1])
        distance()

    gram = gram_ref[...]
    parts = halves(gram)
    mix = LAST[0] * eye + LAST[1] * gram + LAST[2] * product_half(parts, parts)
    basis = product_half(halves(mix), halves(w_ref[...]))
    bias = -slope * jnp.sum(basis[:, n:], axis=1, keepdims=True)
    lead = halves(basis[:, :n])
    for piece in range(PIECES):
        where = slice(piece * chunk, (piece + 1) * chunk)
        projected = product_half(lead, (c_hi[:, where], c_lo[:, where])) + bias
        energy = jnp.sum(projected * projected, axis=0, keepdims=True)
        out_ref[:, where] = 1.0 / (energy / length_ref[:, where] + spectral_floor)


def finish_user(packed, count, grid_index, beams_total):
    n = WIN_BEAMS
    points = grid_index.shape[1]
    vmem = pl.BlockSpec(memory_space=pltpu.VMEM)
    return pl.pallas_call(
        functools.partial(finish_kernel, beams_total),
        out_shape=jax.ShapeDtypeStruct(grid_index.shape, jnp.float32),
        in_specs=[vmem, pl.BlockSpec(memory_space=pltpu.SMEM), vmem],
        out_specs=vmem,
        scratch_shapes=[
            pltpu.VMEM((2 * n, 2 * n), jnp.bfloat16),
            pltpu.VMEM((2 * n, 2 * n), jnp.bfloat16),
            pltpu.VMEM((n, 2 * n), jnp.float32),
            pltpu.VMEM((n, 2 * n), jnp.float32),
            pltpu.VMEM((n, n), jnp.float32),
            pltpu.VMEM((n, points), jnp.bfloat16),
            pltpu.VMEM((n, points), jnp.bfloat16),
            pltpu.VMEM((1, points), jnp.float32),
        ],
        name="finish_user",
    )(packed, count, grid_index)


def local(beam_data, window_count, slot_owner, slot_window, grid_index):
    owners, groups = lax.axis_size("beam"), lax.axis_size("grp")
    slots = slot_window.shape[1]
    x = beam_data.transpose(0, 2, 1)
    packed = exchange(x, window_count, slot_owner[:, :, 0], slot_window, groups, owners, slots)
    return finish_user(packed, window_count, grid_index, beam_data.shape[1] * owners)


def solution(mesh):
    placed = (
        P(None, "beam", "grp"),
        P(("beam", "grp")),
        P(("beam", "grp"), None, None),
        P(("beam", "grp"), None),
        P(("beam", "grp"), None),
    )
    return jax.shard_map(
        local, mesh=mesh, in_specs=placed, out_specs=P(("beam", "grp"), None), check_vma=False
    )
```

```python
import functools

import jax
import jax.numpy as jnp
from jax import lax
from jax.experimental import pallas as pl
from jax.experimental.pallas import tpu as pltpu
from jax.sharding import PartitionSpec as P

WIN_BEAMS = 128
NOISE_DIM = 64
SNAPS = 256
OVERSAMPLE = 32
ITERS = 8
SIDE = 4
MESH = pl.DeviceIdType.MESH

shift_factor = 1.05
spectral_floor = 0.05


def remote(source, target, send_sem, recv_sem, device):
    return pltpu.make_async_remote_copy(
        src_ref=source,
        dst_ref=target,
        send_sem=send_sem,
        recv_sem=recv_sem,
        device_id=device,
        device_id_type=MESH,
    )


def dot_tn(left, right):
    return lax.dot_general(
        left, right, (((0,), (0,)), ((), ())), preferred_element_type=jnp.float32
    )


def exchange_kernel(
    groups, slots, x_hbm, count_ref, owner_hbm, window_hbm, out_ref, x_ref, owner_ref, window_ref, meta_ref, partial, pieces, metas, chosen, blocks,
    ready, sums, piece_send, piece_recv, meta_send, meta_recv, block_send, block_recv, sum_send, sum_recv, local_sem, load_sem,
):
    b, g = lax.axis_index("beam"), lax.axis_index("grp")
    core, x, y = b % 2, b // (2 * SIDE), (b // 2) % SIDE
    windows, rows = blocks.shape[1:3]

    def along(first, second):
        at_x = (x + first * (1 - core) + second * core) % SIDE
        at_y = (y + first * core + second * (1 - core)) % SIDE
        return (at_x * SIDE + at_y) * 2 + core

    partner = b + 1 - 2 * core
    line = [(g + d) % groups for d in range(groups)]
    order = sorted(range(1, groups), key=lambda d: -min(d, groups - d))
    barrier = pltpu.get_barrier_semaphore()
    greeted = [(b, line[d]) for d in order]
    greeted += [(along(d, 0), g) for d in range(1, SIDE)] + [(along(0, d), g) for d in range(1, SIDE)]
    greeted += [(partner, g)]
    for device in greeted:
        pl.semaphore_signal(barrier, inc=1, device_id=device, device_id_type=MESH)

    loads = [
        pltpu.make_async_copy(source, target, load_sem.at[i])
        for i, (source, target) in enumerate(
            [(x_hbm, x_ref), (owner_hbm, owner_ref), (window_hbm, window_ref)]
        )
    ]
    for load in loads:
        load.start()
    for load in loads:
        load.wait()
    lane = lax.broadcasted_iota(jnp.int32, meta_ref.shape, 1)
    meta = jnp.full(meta_ref.shape, -1, jnp.int32)
    for k in range(slots):
        wanted = jnp.where(k < count_ref[0], window_ref[0, k], -1)
        meta = jnp.where(lane == k, owner_ref[0, k], jnp.where(lane == slots + k, wanted, meta))
    meta_ref[...] = meta
    row = lax.broadcasted_iota(jnp.int32, (WIN_BEAMS, WIN_BEAMS), 0)
    col = lax.broadcasted_iota(jnp.int32, (WIN_BEAMS, WIN_BEAMS), 1)
    for w in range(windows):
        real = x_ref[0, :, w * WIN_BEAMS : (w + 1) * WIN_BEAMS]
        imag = x_ref[1, :, w * WIN_BEAMS : (w + 1) * WIN_BEAMS]
        same = dot_tn(real, real) + dot_tn(imag, imag)
        cross = dot_tn(imag, real) - dot_tn(real, imag)
        packed = jnp.where(row <= col, same, cross)
        for s in range(groups):
            partial[s, w] = packed[s * rows : (s + 1) * rows]
    pl.semaphore_wait(barrier, len(greeted))

    sent = []

    def send(*args):
        copy = remote(*args)
        copy.start()
        sent.append(copy)

    for d in order:
        send(partial.at[line[d]], pieces.at[g], piece_send.at[d], piece_recv.at[g], (b, line[d]))
    for d in order:
        send(meta_ref, metas.at[g], meta_send.at[d], meta_recv.at[g], (b, line[d]))
    metas[g] = meta_ref[...]
    own = partial[g]
    for d in reversed(order):
        piece = pieces.at[line[d]]
        remote(piece, piece, piece_send.at[d], piece_recv.at[line[d]], (b, line[d])).wait_recv()
        own = own + pieces[line[d]]
    blocks[b] = own

    count = [0]

    def pass_on(block, device):
        piece = blocks.at[block]
        send(piece, piece, block_send.at[count[0]], block_recv.at[block], (device, g))
        count[0] += 1

    def arrived(block):
        piece = blocks.at[block]
        remote(piece, piece, block_send.at[0], block_recv.at[block], (partner, g)).wait_recv()

    for d in (2, 1, 3):
        pass_on(b, along(d, 0))
    for d in (2, 1, 3):
        pass_on(b, along(0, d))
    pass_on(b, partner)
    for d in range(1, groups):
        remote(meta_ref, metas.at[line[d]], meta_send.at[d], meta_recv.at[line[d]], (b, line[d])).wait_recv()
    fetch = pltpu.make_async_copy(metas, chosen, local_sem)
    fetch.start()
    for e in (1, 3, 2):
        block = along(e, 0)
        arrived(block)
        for d in (2, 1, 3):
            pass_on(block, along(0, d))
        pass_on(block, partner)
    for e in (0, 1, 3, 2):
        for d in (1, 3, 2):
            block = along(e, d)
            arrived(block)
            pass_on(block, partner)
    fetch.wait()
    for i in range(SIDE * SIDE):
        arrived(2 * i + 1 - core)

    for d in order + [0]:
        total = jnp.zeros((rows, WIN_BEAMS), jnp.float32)
        for k in range(slots):
            wanted = chosen[line[d], 0, slots + k]
            weight = jnp.where(wanted >= 0, 1.0, 0.0)
            total = total + weight * blocks[chosen[line[d], 0, k], jnp.maximum(wanted, 0)]
        if d == 0:
            out_ref[g] = total
        else:
            ready[d] = total
            send(ready.at[d], sums.at[g], sum_send.at[d], sum_recv.at[g], (b, line[d]))
    for d in range(1, groups):
        piece = sums.at[line[d]]
        remote(piece, piece, sum_send.at[d], sum_recv.at[line[d]], (b, line[d])).wait_recv()
        out_ref[line[d]] = sums[line[d]]
    for copy in sent:
        copy.wait_send()


def exchange(x, count, owner, window, groups, owners, slots):
    windows, rows = x.shape[2] // WIN_BEAMS, WIN_BEAMS // groups
    vmem, smem = pl.BlockSpec(memory_space=pltpu.VMEM), pl.BlockSpec(memory_space=pltpu.SMEM)
    hbm = pl.BlockSpec(memory_space=pltpu.HBM)
    meta = (8, 128)
    dma = pltpu.SemaphoreType.DMA
    forwards = 2 * (SIDE - 1) + 1 + (SIDE - 1) * SIDE + SIDE * (SIDE - 1)
    return pl.pallas_call(
        functools.partial(exchange_kernel, groups, slots),
        out_shape=jax.ShapeDtypeStruct((groups, rows, WIN_BEAMS), jnp.float32),
        in_specs=[hbm, smem, hbm, hbm],
        out_specs=vmem,
        scratch_shapes=[
            pltpu.VMEM(x.shape, x.dtype),
            pltpu.SMEM(owner.shape, owner.dtype),
            pltpu.SMEM(window.shape, window.dtype),
            pltpu.VMEM(meta, jnp.int32),
            pltpu.VMEM((groups, windows, rows, WIN_BEAMS), jnp.float32),
            pltpu.VMEM((groups, windows, rows, WIN_BEAMS), jnp.float32),
            pltpu.VMEM((groups,) + meta, jnp.int32),
            pltpu.SMEM((groups,) + meta, jnp.int32),
            pltpu.VMEM((owners, windows, rows, WIN_BEAMS), jnp.float32),
            pltpu.VMEM((groups, rows, WIN_BEAMS), jnp.float32),
            pltpu.VMEM((groups, rows, WIN_BEAMS), jnp.float32),
            dma((groups,)),
            dma((groups,)),
            dma((groups,)),
            dma((groups,)),
            dma((forwards,)),
            dma((owners,)),
            dma((groups,)),
            dma((groups,)),
            dma,
            dma((3,)),
        ],
        compiler_params=pltpu.CompilerParams(collective_id=0, has_side_effects=True),
        name="exchange",
    )(x, count, owner, window).reshape(WIN_BEAMS, WIN_BEAMS)


FAST = (2.4, -1.45, 0.0)
GROW = (3.4445, -4.7750, 2.0315)
CLOSE = ((3.109266, -3.792034, 1.535381), (1.90467, -1.282586, 0.3782733))
LAST = (1.875, -1.25, 0.375)
NEAR = 0.016
PIECES = 8


def halves(value):
    high = value.astype(jnp.bfloat16)
    return high, (value - high.astype(jnp.float32)).astype(jnp.bfloat16)


def dot(left, right):
    return jnp.dot(left, right, preferred_element_type=jnp.float32)


def dot_nt(left, right):
    return lax.dot_general(
        left, right, (((1,), (1,)), ((), ())), preferred_element_type=jnp.float32
    )


def product(left, right):
    return dot(left[0], right[0]) + (dot(left[0], right[1]) + dot(left[1], right[0]))


def product_half(left, right):
    both = dot(
        jnp.concatenate([left[0], left[1]], axis=1),
        jnp.concatenate([right[0], right[0]], axis=0),
    )
    return both + dot(left[0], right[1])


def whole(top):
    n = WIN_BEAMS
    return jnp.concatenate([top, jnp.concatenate([-top[:, n:], top[:, :n]], axis=1)], axis=0)


def finish_kernel(
    beams_total, packed_ref, count_ref, grid_ref, out_ref, a_hi, a_lo, b_hi, b_lo, start_ref, w_ref, gram_ref, c_hi, c_lo, length_ref
):
    n = WIN_BEAMS
    chunk = grid_ref.shape[1] // PIECES
    slope = jnp.pi / beams_total
    row = lax.broadcasted_iota(jnp.int32, (n, n), 0)
    col = lax.broadcasted_iota(jnp.int32, (n, n), 1)
    packed = packed_ref[...]
    flipped = packed.T
    same = jnp.where(row <= col, packed, flipped)
    imag = jnp.where(row > col, packed, jnp.where(row < col, -flipped, 0.0))
    scale = jnp.full((1, 1), 1.0, jnp.float32) / (count_ref[0].astype(jnp.float32) * SNAPS)
    top = jnp.concatenate([same, -imag], axis=1) * scale
    square = product(halves(top), halves(whole(top)))
    fourth = product(halves(square), halves(whole(square)))
    power = 2.0 * jnp.sum(fourth * fourth, axis=(0, 1), keepdims=True)
    shift = shift_factor * jnp.sqrt(jnp.sqrt(jnp.sqrt(power)))
    row2 = lax.broadcasted_iota(jnp.int32, (n, 2 * n), 0)
    col2 = lax.broadcasted_iota(jnp.int32, (n, 2 * n), 1)
    shifted = whole(jnp.where(row2 == col2, 1.0, 0.0) - top / shift)
    hi, lo = halves(shifted)
    a_hi[...] = hi
    a_lo[...] = lo
    start_ref[...] = jnp.concatenate([shifted[:NOISE_DIM], shifted[n : n + NOISE_DIM]], axis=0)
    twice = whole(product((hi[:n], lo[:n]), (hi, lo)))
    hi, lo = halves(twice)
    b_hi[...] = hi
    b_lo[...] = lo
    w_ref[...] = jnp.concatenate([twice[:NOISE_DIM], twice[n : n + NOISE_DIM]], axis=0)
    eye = jnp.where(row == col, 1.0, 0.0)

    def steer(piece):
        where = pl.ds(pl.multiple_of(piece * chunk, chunk), chunk)
        position = (grid_ref[:, where].astype(jnp.float32) + 0.5) / OVERSAMPLE
        offset = position - lax.broadcasted_iota(jnp.int32, (n, chunk), 0).astype(jnp.float32)
        angle = (slope * offset) * (slope * offset)
        series = 1.0 / 3.0 + angle * (1.0 / 45.0 + angle * (2.0 / 945.0))
        cot = 1.0 / offset - (slope * slope * offset) * series
        high, low = halves(cot)
        c_hi[:, where] = high
        c_lo[:, where] = low
        length_ref[:, where] = jnp.sum(cot * cot, axis=0, keepdims=True) + n * slope * slope

    def step(coefs, operator=None):
        a, b, c = coefs
        parts = halves(w_ref[...])
        gram = dot_nt(parts[0], parts[0])
        mix = a * eye + b * gram
        if c:
            low = gram.astype(jnp.bfloat16)
            mix = mix + c * dot(low, low)
        moved = halves(product(parts, (operator[0][...], operator[1][...]))) if operator else parts
        w_ref[...] = product_half(halves(mix), moved)

    def distance():
        parts = halves(w_ref[...])
        cross = dot_nt(parts[0], parts[1])
        gram = dot_nt(parts[0], parts[0]) + (cross + dot_nt(parts[1], parts[0]))
        gram_ref[...] = gram
        return jnp.sum((gram - eye) * (gram - eye))

    @pl.loop(0, ITERS // 2 - 1)
    def _(i):
        step(FAST, (b_hi, b_lo))
        steer(2 * i)
        steer(2 * i + 1)

    @pl.loop(ITERS - 2, PIECES)
    def _(i):
        step(FAST)
        steer(i)

    step(CLOSE[0])
    step(CLOSE[1])
    off = distance()

    @pl.when(jnp.logical_not(off < NEAR))
    def _():
        w_ref[...] = start_ref[...]

        @pl.loop(0, ITERS - 1)
        def _(_):
            step(GROW)
            step(CLOSE[0])
            step(CLOSE[1], (a_hi, a_lo))

        step(GROW)
        step(CLOSE[0])
        step(CLOSE[1])
        distance()

    gram = gram_ref[...]
    parts = halves(gram)
    mix = LAST[0] * eye + LAST[1] * gram + LAST[2] * product_half(parts, parts)
    basis = product_half(halves(mix), halves(w_ref[...]))
    bias = -slope * jnp.sum(basis[:, n:], axis=1, keepdims=True)
    lead = halves(basis[:, :n])
    for piece in range(PIECES):
        where = slice(piece * chunk, (piece + 1) * chunk)
        projected = product_half(lead, (c_hi[:, where], c_lo[:, where])) + bias
        energy = jnp.sum(projected * projected, axis=0, keepdims=True)
        out_ref[:, where] = 1.0 / (energy / length_ref[:, where] + spectral_floor)


def finish_user(packed, count, grid_index, beams_total):
    n = WIN_BEAMS
    points = grid_index.shape[1]
    vmem = pl.BlockSpec(memory_space=pltpu.VMEM)
    return pl.pallas_call(
        functools.partial(finish_kernel, beams_total),
        out_shape=jax.ShapeDtypeStruct(grid_index.shape, jnp.float32),
        in_specs=[vmem, pl.BlockSpec(memory_space=pltpu.SMEM), vmem],
        out_specs=vmem,
        scratch_shapes=[
            pltpu.VMEM((2 * n, 2 * n), jnp.bfloat16),
            pltpu.VMEM((2 * n, 2 * n), jnp.bfloat16),
            pltpu.VMEM((2 * n, 2 * n), jnp.bfloat16),
            pltpu.VMEM((2 * n, 2 * n), jnp.bfloat16),
            pltpu.VMEM((n, 2 * n), jnp.float32),
            pltpu.VMEM((n, 2 * n), jnp.float32),
            pltpu.VMEM((n, n), jnp.float32),
            pltpu.VMEM((n, points), jnp.bfloat16),
            pltpu.VMEM((n, points), jnp.bfloat16),
            pltpu.VMEM((1, points), jnp.float32),
        ],
        name="finish_user",
    )(packed, count, grid_index)


def local(beam_data, window_count, slot_owner, slot_window, grid_index):
    owners, groups = lax.axis_size("beam"), lax.axis_size("grp")
    slots = slot_window.shape[1]
    x = beam_data.transpose(0, 2, 1)
    packed = exchange(x, window_count, slot_owner[:, :, 0], slot_window, groups, owners, slots)
    return finish_user(packed, window_count, grid_index, beam_data.shape[1] * owners)


def solution(mesh):
    placed = (
        P(None, "beam", "grp"),
        P(("beam", "grp")),
        P(("beam", "grp"), None, None),
        P(("beam", "grp"), None),
        P(("beam", "grp"), None),
    )
    return jax.shard_map(
        local, mesh=mesh, in_specs=placed, out_specs=P(("beam", "grp"), None), check_vma=False
    )
```

```python
import functools

import jax
import jax.numpy as jnp
from jax import lax
from jax.experimental import pallas as pl
from jax.experimental.pallas import tpu as pltpu
from jax.sharding import PartitionSpec as P

WIN_BEAMS = 128
NOISE_DIM = 64
SNAPS = 256
OVERSAMPLE = 32
ITERS = 8
SIDE = 4
MESH = pl.DeviceIdType.MESH

shift_factor = 1.05
spectral_floor = 0.05


def remote(source, target, send_sem, recv_sem, device):
    return pltpu.make_async_remote_copy(
        src_ref=source,
        dst_ref=target,
        send_sem=send_sem,
        recv_sem=recv_sem,
        device_id=device,
        device_id_type=MESH,
    )


def dot_tn(left, right):
    return lax.dot_general(
        left, right, (((0,), (0,)), ((), ())), preferred_element_type=jnp.float32
    )


def exchange_kernel(
    groups, slots, x_hbm, count_ref, owner_hbm, window_hbm, out_ref, x_ref, owner_ref, window_ref, meta_ref, partial, pieces, metas, chosen, blocks,
    ready, sums, piece_send, piece_recv, meta_send, meta_recv, block_send, block_recv, sum_send, sum_recv, local_sem, load_sem,
):
    b, g = lax.axis_index("beam"), lax.axis_index("grp")
    core, x, y = b % 2, b // (2 * SIDE), (b // 2) % SIDE
    windows, rows = blocks.shape[1:3]

    def along(first, second):
        at_x = (x + first * (1 - core) + second * core) % SIDE
        at_y = (y + first * core + second * (1 - core)) % SIDE
        return (at_x * SIDE + at_y) * 2 + core

    partner = b + 1 - 2 * core
    line = [(g + d) % groups for d in range(groups)]
    order = sorted(range(1, groups), key=lambda d: -min(d, groups - d))
    barrier = pltpu.get_barrier_semaphore()
    greeted = [(b, line[d]) for d in order]
    steps = [(e, d) for e in range(SIDE) for d in range(SIDE) if e or d]
    steps.sort(key=lambda s: -min(s[0], SIDE - s[0]) - min(s[1], SIDE - s[1]))
    greeted += [(along(e, d), g) for e, d in steps]
    greeted += [(partner, g)]
    for device in greeted:
        pl.semaphore_signal(barrier, inc=1, device_id=device, device_id_type=MESH)

    loads = [
        pltpu.make_async_copy(source, target, load_sem.at[i])
        for i, (source, target) in enumerate(
            [(x_hbm, x_ref), (owner_hbm, owner_ref), (window_hbm, window_ref)]
        )
    ]
    for load in loads:
        load.start()
    for load in loads:
        load.wait()
    lane = lax.broadcasted_iota(jnp.int32, meta_ref.shape, 1)
    meta = jnp.full(meta_ref.shape, -1, jnp.int32)
    for k in range(slots):
        wanted = jnp.where(k < count_ref[0], window_ref[0, k], -1)
        meta = jnp.where(lane == k, owner_ref[0, k], jnp.where(lane == slots + k, wanted, meta))
    meta_ref[...] = meta
    row = lax.broadcasted_iota(jnp.int32, (WIN_BEAMS, WIN_BEAMS), 0)
    col = lax.broadcasted_iota(jnp.int32, (WIN_BEAMS, WIN_BEAMS), 1)
    for w in range(windows):
        real = x_ref[0, :, w * WIN_BEAMS : (w + 1) * WIN_BEAMS]
        imag = x_ref[1, :, w * WIN_BEAMS : (w + 1) * WIN_BEAMS]
        same = dot_tn(real, real) + dot_tn(imag, imag)
        cross = dot_tn(imag, real) - dot_tn(real, imag)
        packed = jnp.where(row <= col, same, cross)
        for s in range(groups):
            partial[s, w] = packed[s * rows : (s + 1) * rows]
    pl.semaphore_wait(barrier, len(greeted))

    sent = []

    def send(*args):
        copy = remote(*args)
        copy.start()
        sent.append(copy)

    for d in order:
        send(partial.at[line[d]], pieces.at[g], piece_send.at[d], piece_recv.at[g], (b, line[d]))
    for d in order:
        send(meta_ref, metas.at[g], meta_send.at[d], meta_recv.at[g], (b, line[d]))
    metas[g] = meta_ref[...]
    own = partial[g]
    for d in reversed(order):
        piece = pieces.at[line[d]]
        remote(piece, piece, piece_send.at[d], piece_recv.at[line[d]], (b, line[d])).wait_recv()
        own = own + pieces[line[d]]
    blocks[b] = own

    count = [0]

    def pass_on(block, device):
        piece = blocks.at[block]
        send(piece, piece, block_send.at[count[0]], block_recv.at[block], (device, g))
        count[0] += 1

    def arrived(block):
        piece = blocks.at[block]
        remote(piece, piece, block_send.at[0], block_recv.at[block], (partner, g)).wait_recv()

    pass_on(b, partner)
    for e, d in steps:
        pass_on(b, along(e, d))
    for d in range(1, groups):
        remote(meta_ref, metas.at[line[d]], meta_send.at[d], meta_recv.at[line[d]], (b, line[d])).wait_recv()
    fetch = pltpu.make_async_copy(metas, chosen, local_sem)
    fetch.start()
    for e, d in reversed(steps):
        block = along(e, d)
        arrived(block)
        pass_on(block, partner)
    fetch.wait()
    for i in range(SIDE * SIDE):
        arrived(2 * i + 1 - core)

    for d in order + [0]:
        total = jnp.zeros((rows, WIN_BEAMS), jnp.float32)
        for k in range(slots):
            wanted = chosen[line[d], 0, slots + k]
            weight = jnp.where(wanted >= 0, 1.0, 0.0)
            total = total + weight * blocks[chosen[line[d], 0, k], jnp.maximum(wanted, 0)]
        if d == 0:
            out_ref[g] = total
        else:
            ready[d] = total
            send(ready.at[d], sums.at[g], sum_send.at[d], sum_recv.at[g], (b, line[d]))
    for d in range(1, groups):
        piece = sums.at[line[d]]
        remote(piece, piece, sum_send.at[d], sum_recv.at[line[d]], (b, line[d])).wait_recv()
        out_ref[line[d]] = sums[line[d]]
    for copy in sent:
        copy.wait_send()


def exchange(x, count, owner, window, groups, owners, slots):
    windows, rows = x.shape[2] // WIN_BEAMS, WIN_BEAMS // groups
    vmem, smem = pl.BlockSpec(memory_space=pltpu.VMEM), pl.BlockSpec(memory_space=pltpu.SMEM)
    hbm = pl.BlockSpec(memory_space=pltpu.HBM)
    meta = (8, 128)
    dma = pltpu.SemaphoreType.DMA
    forwards = 2 * SIDE * SIDE - 1
    return pl.pallas_call(
        functools.partial(exchange_kernel, groups, slots),
        out_shape=jax.ShapeDtypeStruct((groups, rows, WIN_BEAMS), jnp.float32),
        in_specs=[hbm, smem, hbm, hbm],
        out_specs=vmem,
        scratch_shapes=[
            pltpu.VMEM(x.shape, x.dtype),
            pltpu.SMEM(owner.shape, owner.dtype),
            pltpu.SMEM(window.shape, window.dtype),
            pltpu.VMEM(meta, jnp.int32),
            pltpu.VMEM((groups, windows, rows, WIN_BEAMS), jnp.float32),
            pltpu.VMEM((groups, windows, rows, WIN_BEAMS), jnp.float32),
            pltpu.VMEM((groups,) + meta, jnp.int32),
            pltpu.SMEM((groups,) + meta, jnp.int32),
            pltpu.VMEM((owners, windows, rows, WIN_BEAMS), jnp.float32),
            pltpu.VMEM((groups, rows, WIN_BEAMS), jnp.float32),
            pltpu.VMEM((groups, rows, WIN_BEAMS), jnp.float32),
            dma((groups,)),
            dma((groups,)),
            dma((groups,)),
            dma((groups,)),
            dma((forwards,)),
            dma((owners,)),
            dma((groups,)),
            dma((groups,)),
            dma,
            dma((3,)),
        ],
        compiler_params=pltpu.CompilerParams(collective_id=0, has_side_effects=True),
        name="exchange",
    )(x, count, owner, window).reshape(WIN_BEAMS, WIN_BEAMS)


FAST = (2.4, -1.45, 0.0)
GROW = (3.4445, -4.7750, 2.0315)
CLOSE = ((3.109266, -3.792034, 1.535381), (1.90467, -1.282586, 0.3782733))
LAST = (1.875, -1.25, 0.375)
NEAR = 0.016
PIECES = 8


def halves(value):
    high = value.astype(jnp.bfloat16)
    return high, (value - high.astype(jnp.float32)).astype(jnp.bfloat16)


def dot(left, right):
    return jnp.dot(left, right, preferred_element_type=jnp.float32)


def dot_nt(left, right):
    return lax.dot_general(
        left, right, (((1,), (1,)), ((), ())), preferred_element_type=jnp.float32
    )


def product(left, right):
    return dot(left[0], right[0]) + (dot(left[0], right[1]) + dot(left[1], right[0]))


def product_half(left, right):
    both = dot(
        jnp.concatenate([left[0], left[1]], axis=1),
        jnp.concatenate([right[0], right[0]], axis=0),
    )
    return both + dot(left[0], right[1])


def whole(top):
    n = WIN_BEAMS
    return jnp.concatenate([top, jnp.concatenate([-top[:, n:], top[:, :n]], axis=1)], axis=0)


def finish_kernel(
    beams_total, packed_ref, count_ref, grid_ref, out_ref, a_hi, a_lo, b_hi, b_lo, start_ref, w_ref, gram_ref, c_hi, c_lo, length_ref
):
    n = WIN_BEAMS
    chunk = grid_ref.shape[1] // PIECES
    slope = jnp.pi / beams_total
    row = lax.broadcasted_iota(jnp.int32, (n, n), 0)
    col = lax.broadcasted_iota(jnp.int32, (n, n), 1)
    packed = packed_ref[...]
    flipped = packed.T
    same = jnp.where(row <= col, packed, flipped)
    imag = jnp.where(row > col, packed, jnp.where(row < col, -flipped, 0.0))
    scale = jnp.full((1, 1), 1.0, jnp.float32) / (count_ref[0].astype(jnp.float32) * SNAPS)
    top = jnp.concatenate([same, -imag], axis=1) * scale
    square = product(halves(top), halves(whole(top)))
    fourth = product(halves(square), halves(whole(square)))
    power = 2.0 * jnp.sum(fourth * fourth, axis=(0, 1), keepdims=True)
    shift = shift_factor * jnp.sqrt(jnp.sqrt(jnp.sqrt(power)))
    row2 = lax.broadcasted_iota(jnp.int32, (n, 2 * n), 0)
    col2 = lax.broadcasted_iota(jnp.int32, (n, 2 * n), 1)
    shifted = whole(jnp.where(row2 == col2, 1.0, 0.0) - top / shift)
    hi, lo = halves(shifted)
    a_hi[...] = hi
    a_lo[...] = lo
    start_ref[...] = jnp.concatenate([shifted[:NOISE_DIM], shifted[n : n + NOISE_DIM]], axis=0)
    twice = whole(product((hi[:n], lo[:n]), (hi, lo)))
    hi, lo = halves(twice)
    b_hi[...] = hi
    b_lo[...] = lo
    w_ref[...] = jnp.concatenate([twice[:NOISE_DIM], twice[n : n + NOISE_DIM]], axis=0)
    eye = jnp.where(row == col, 1.0, 0.0)

    def steer(piece):
        where = pl.ds(pl.multiple_of(piece * chunk, chunk), chunk)
        position = (grid_ref[:, where].astype(jnp.float32) + 0.5) / OVERSAMPLE
        offset = position - lax.broadcasted_iota(jnp.int32, (n, chunk), 0).astype(jnp.float32)
        angle = (slope * offset) * (slope * offset)
        series = 1.0 / 3.0 + angle * (1.0 / 45.0 + angle * (2.0 / 945.0))
        cot = 1.0 / offset - (slope * slope * offset) * series
        high, low = halves(cot)
        c_hi[:, where] = high
        c_lo[:, where] = low
        length_ref[:, where] = jnp.sum(cot * cot, axis=0, keepdims=True) + n * slope * slope

    def step(coefs, operator=None):
        a, b, c = coefs
        parts = halves(w_ref[...])
        gram = dot_nt(parts[0], parts[0])
        mix = a * eye + b * gram
        if c:
            low = gram.astype(jnp.bfloat16)
            mix = mix + c * dot(low, low)
        moved = halves(product(parts, (operator[0][...], operator[1][...]))) if operator else parts
        w_ref[...] = product_half(halves(mix), moved)

    def distance():
        parts = halves(w_ref[...])
        cross = dot_nt(parts[0], parts[1])
        gram = dot_nt(parts[0], parts[0]) + (cross + dot_nt(parts[1], parts[0]))
        gram_ref[...] = gram
        return jnp.sum((gram - eye) * (gram - eye))

    @pl.loop(0, ITERS // 2 - 1)
    def _(i):
        step(FAST, (b_hi, b_lo))
        steer(2 * i)
        steer(2 * i + 1)

    @pl.loop(ITERS - 2, PIECES)
    def _(i):
        step(FAST)
        steer(i)

    step(CLOSE[0])
    step(CLOSE[1])
    off = distance()

    @pl.when(jnp.logical_not(off < NEAR))
    def _():
        w_ref[...] = start_ref[...]

        @pl.loop(0, ITERS - 1)
        def _(_):
            step(GROW)
            step(CLOSE[0])
            step(CLOSE[1], (a_hi, a_lo))

        step(GROW)
        step(CLOSE[0])
        step(CLOSE[1])
        distance()

    gram = gram_ref[...]
    parts = halves(gram)
    mix = LAST[0] * eye + LAST[1] * gram + LAST[2] * product_half(parts, parts)
    basis = product_half(halves(mix), halves(w_ref[...]))
    bias = -slope * jnp.sum(basis[:, n:], axis=1, keepdims=True)
    lead = halves(basis[:, :n])
    for piece in range(PIECES):
        where = slice(piece * chunk, (piece + 1) * chunk)
        projected = product_half(lead, (c_hi[:, where], c_lo[:, where])) + bias
        energy = jnp.sum(projected * projected, axis=0, keepdims=True)
        out_ref[:, where] = 1.0 / (energy / length_ref[:, where] + spectral_floor)


def finish_user(packed, count, grid_index, beams_total):
    n = WIN_BEAMS
    points = grid_index.shape[1]
    vmem = pl.BlockSpec(memory_space=pltpu.VMEM)
    return pl.pallas_call(
        functools.partial(finish_kernel, beams_total),
        out_shape=jax.ShapeDtypeStruct(grid_index.shape, jnp.float32),
        in_specs=[vmem, pl.BlockSpec(memory_space=pltpu.SMEM), vmem],
        out_specs=vmem,
        scratch_shapes=[
            pltpu.VMEM((2 * n, 2 * n), jnp.bfloat16),
            pltpu.VMEM((2 * n, 2 * n), jnp.bfloat16),
            pltpu.VMEM((2 * n, 2 * n), jnp.bfloat16),
            pltpu.VMEM((2 * n, 2 * n), jnp.bfloat16),
            pltpu.VMEM((n, 2 * n), jnp.float32),
            pltpu.VMEM((n, 2 * n), jnp.float32),
            pltpu.VMEM((n, n), jnp.float32),
            pltpu.VMEM((n, points), jnp.bfloat16),
            pltpu.VMEM((n, points), jnp.bfloat16),
            pltpu.VMEM((1, points), jnp.float32),
        ],
        name="finish_user",
    )(packed, count, grid_index)


def local(beam_data, window_count, slot_owner, slot_window, grid_index):
    owners, groups = lax.axis_size("beam"), lax.axis_size("grp")
    slots = slot_window.shape[1]
    x = beam_data.transpose(0, 2, 1)
    packed = exchange(x, window_count, slot_owner[:, :, 0], slot_window, groups, owners, slots)
    return finish_user(packed, window_count, grid_index, beam_data.shape[1] * owners)


def solution(mesh):
    placed = (
        P(None, "beam", "grp"),
        P(("beam", "grp")),
        P(("beam", "grp"), None, None),
        P(("beam", "grp"), None),
        P(("beam", "grp"), None),
    )
    return jax.shard_map(
        local, mesh=mesh, in_specs=placed, out_specs=P(("beam", "grp"), None), check_vma=False
    )
```

```python
import functools

import jax
import jax.numpy as jnp
from jax import lax
from jax.experimental import pallas as pl
from jax.experimental.pallas import tpu as pltpu
from jax.sharding import PartitionSpec as P

WIN_BEAMS = 128
NOISE_DIM = 64
SNAPS = 256
OVERSAMPLE = 32
ITERS = 8
SIDE = 4
MESH = pl.DeviceIdType.MESH

shift_factor = 1.05
spectral_floor = 0.05


def remote(source, target, send_sem, recv_sem, device):
    return pltpu.make_async_remote_copy(
        src_ref=source,
        dst_ref=target,
        send_sem=send_sem,
        recv_sem=recv_sem,
        device_id=device,
        device_id_type=MESH,
    )


def dot_tn(left, right):
    return lax.dot_general(
        left, right, (((0,), (0,)), ((), ())), preferred_element_type=jnp.float32
    )


def exchange_kernel(
    groups, slots, x_hbm, count_ref, owner_hbm, window_hbm, out_ref, x_ref, owner_ref, window_ref, meta_ref, partial, pieces, metas, chosen, blocks,
    ready, sums, piece_send, piece_recv, meta_send, meta_recv, block_send, block_recv, sum_send, sum_recv, local_sem, load_sem,
):
    b, g = lax.axis_index("beam"), lax.axis_index("grp")
    core, x, y = b % 2, b // (2 * SIDE), (b // 2) % SIDE
    windows, rows = blocks.shape[1:3]

    def along(first, second):
        at_x = (x + first * (1 - core) + second * core) % SIDE
        at_y = (y + first * core + second * (1 - core)) % SIDE
        return (at_x * SIDE + at_y) * 2 + core

    partner = b + 1 - 2 * core
    line = [(g + d) % groups for d in range(groups)]
    order = sorted(range(1, groups), key=lambda d: -min(d, groups - d))
    barrier = pltpu.get_barrier_semaphore()
    greeted = [(b, line[d]) for d in order]
    steps = [(e, d) for e in range(SIDE) for d in range(SIDE) if e or d]
    steps.sort(key=lambda s: -min(s[0], SIDE - s[0]) - min(s[1], SIDE - s[1]))
    greeted += [(along(e, d), g) for e, d in steps]
    greeted += [(partner, g)]
    for device in greeted:
        pl.semaphore_signal(barrier, inc=1, device_id=device, device_id_type=MESH)

    loads = [
        pltpu.make_async_copy(source, target, load_sem.at[i])
        for i, (source, target) in enumerate(
            [(x_hbm, x_ref), (owner_hbm, owner_ref), (window_hbm, window_ref)]
        )
    ]
    for load in loads:
        load.start()
    for load in loads:
        load.wait()
    lane = lax.broadcasted_iota(jnp.int32, meta_ref.shape, 1)
    meta = jnp.full(meta_ref.shape, -1, jnp.int32)
    for k in range(slots):
        wanted = jnp.where(k < count_ref[0], window_ref[0, k], -1)
        meta = jnp.where(lane == k, owner_ref[0, k], jnp.where(lane == slots + k, wanted, meta))
    meta_ref[...] = meta
    row = lax.broadcasted_iota(jnp.int32, (WIN_BEAMS, WIN_BEAMS), 0)
    col = lax.broadcasted_iota(jnp.int32, (WIN_BEAMS, WIN_BEAMS), 1)
    for w in range(windows):
        real = x_ref[0, :, w * WIN_BEAMS : (w + 1) * WIN_BEAMS]
        imag = x_ref[1, :, w * WIN_BEAMS : (w + 1) * WIN_BEAMS]
        same = dot_tn(real, real) + dot_tn(imag, imag)
        cross = dot_tn(imag, real) - dot_tn(real, imag)
        packed = jnp.where(row <= col, same, cross)
        for s in range(groups):
            partial[s, w] = packed[s * rows : (s + 1) * rows]
    pl.semaphore_wait(barrier, len(greeted))

    sent = []

    def send(*args):
        copy = remote(*args)
        copy.start()
        sent.append(copy)

    halves_of = [pl.ds(p * (windows // 2), windows // 2) for p in range(2)]
    for p, part in enumerate(halves_of):
        for d in order:
            target = pieces.at[g, part]
            send(partial.at[line[d], part], target, piece_send.at[p, d], piece_recv.at[p, g], (b, line[d]))
    for d in order:
        send(meta_ref, metas.at[g], meta_send.at[d], meta_recv.at[g], (b, line[d]))
    metas[g] = meta_ref[...]

    count = [0]

    def pass_on(p, block, device):
        piece = blocks.at[block, halves_of[p]]
        send(piece, piece, block_send.at[count[0]], block_recv.at[p, block], (device, g))
        count[0] += 1

    def arrived(p, block):
        piece = blocks.at[block, halves_of[p]]
        remote(piece, piece, block_send.at[0], block_recv.at[p, block], (partner, g)).wait_recv()

    for p, part in enumerate(halves_of):
        own = partial[g, part]
        for d in reversed(order):
            piece = pieces.at[line[d], part]
            remote(piece, piece, piece_send.at[p, d], piece_recv.at[p, line[d]], (b, line[d])).wait_recv()
            own = own + pieces[line[d], part]
        blocks[b, part] = own
        pass_on(p, b, partner)
        for e, d in steps:
            pass_on(p, b, along(e, d))
    for d in range(1, groups):
        remote(meta_ref, metas.at[line[d]], meta_send.at[d], meta_recv.at[line[d]], (b, line[d])).wait_recv()
    fetch = pltpu.make_async_copy(metas, chosen, local_sem)
    fetch.start()
    for p in range(2):
        for e, d in reversed(steps):
            block = along(e, d)
            arrived(p, block)
            pass_on(p, block, partner)
    fetch.wait()
    for p in range(2):
        for i in range(SIDE * SIDE):
            arrived(p, 2 * i + 1 - core)

    for d in order + [0]:
        total = jnp.zeros((rows, WIN_BEAMS), jnp.float32)
        for k in range(slots):
            wanted = chosen[line[d], 0, slots + k]
            weight = jnp.where(wanted >= 0, 1.0, 0.0)
            total = total + weight * blocks[chosen[line[d], 0, k], jnp.maximum(wanted, 0)]
        if d == 0:
            out_ref[g] = total
        else:
            ready[d] = total
            send(ready.at[d], sums.at[g], sum_send.at[d], sum_recv.at[g], (b, line[d]))
    for d in range(1, groups):
        piece = sums.at[line[d]]
        remote(piece, piece, sum_send.at[d], sum_recv.at[line[d]], (b, line[d])).wait_recv()
        out_ref[line[d]] = sums[line[d]]
    for copy in sent:
        copy.wait_send()


def exchange(x, count, owner, window, groups, owners, slots):
    windows, rows = x.shape[2] // WIN_BEAMS, WIN_BEAMS // groups
    vmem, smem = pl.BlockSpec(memory_space=pltpu.VMEM), pl.BlockSpec(memory_space=pltpu.SMEM)
    hbm = pl.BlockSpec(memory_space=pltpu.HBM)
    meta = (8, 128)
    dma = pltpu.SemaphoreType.DMA
    forwards = 2 * (2 * SIDE * SIDE - 1)
    return pl.pallas_call(
        functools.partial(exchange_kernel, groups, slots),
        out_shape=jax.ShapeDtypeStruct((groups, rows, WIN_BEAMS), jnp.float32),
        in_specs=[hbm, smem, hbm, hbm],
        out_specs=vmem,
        scratch_shapes=[
            pltpu.VMEM(x.shape, x.dtype),
            pltpu.SMEM(owner.shape, owner.dtype),
            pltpu.SMEM(window.shape, window.dtype),
            pltpu.VMEM(meta, jnp.int32),
            pltpu.VMEM((groups, windows, rows, WIN_BEAMS), jnp.float32),
            pltpu.VMEM((groups, windows, rows, WIN_BEAMS), jnp.float32),
            pltpu.VMEM((groups,) + meta, jnp.int32),
            pltpu.SMEM((groups,) + meta, jnp.int32),
            pltpu.VMEM((owners, windows, rows, WIN_BEAMS), jnp.float32),
            pltpu.VMEM((groups, rows, WIN_BEAMS), jnp.float32),
            pltpu.VMEM((groups, rows, WIN_BEAMS), jnp.float32),
            dma((2, groups)),
            dma((2, groups)),
            dma((groups,)),
            dma((groups,)),
            dma((forwards,)),
            dma((2, owners)),
            dma((groups,)),
            dma((groups,)),
            dma,
            dma((3,)),
        ],
        compiler_params=pltpu.CompilerParams(collective_id=0, has_side_effects=True),
        name="exchange",
    )(x, count, owner, window).reshape(WIN_BEAMS, WIN_BEAMS)


FAST = (2.4, -1.45, 0.0)
GROW = (3.4445, -4.7750, 2.0315)
CLOSE = ((3.109266, -3.792034, 1.535381), (1.90467, -1.282586, 0.3782733))
LAST = (1.875, -1.25, 0.375)
NEAR = 0.016
PIECES = 8


def halves(value):
    high = value.astype(jnp.bfloat16)
    return high, (value - high.astype(jnp.float32)).astype(jnp.bfloat16)


def dot(left, right):
    return jnp.dot(left, right, preferred_element_type=jnp.float32)


def dot_nt(left, right):
    return lax.dot_general(
        left, right, (((1,), (1,)), ((), ())), preferred_element_type=jnp.float32
    )


def product(left, right):
    return dot(left[0], right[0]) + (dot(left[0], right[1]) + dot(left[1], right[0]))


def product_half(left, right):
    both = dot(
        jnp.concatenate([left[0], left[1]], axis=1),
        jnp.concatenate([right[0], right[0]], axis=0),
    )
    return both + dot(left[0], right[1])


def whole(top):
    n = WIN_BEAMS
    return jnp.concatenate([top, jnp.concatenate([-top[:, n:], top[:, :n]], axis=1)], axis=0)


def finish_kernel(
    beams_total, packed_ref, count_ref, grid_ref, out_ref, a_hi, a_lo, b_hi, b_lo, start_ref, w_ref, gram_ref, c_hi, c_lo, length_ref
):
    n = WIN_BEAMS
    chunk = grid_ref.shape[1] // PIECES
    slope = jnp.pi / beams_total
    row = lax.broadcasted_iota(jnp.int32, (n, n), 0)
    col = lax.broadcasted_iota(jnp.int32, (n, n), 1)
    packed = packed_ref[...]
    flipped = packed.T
    same = jnp.where(row <= col, packed, flipped)
    imag = jnp.where(row > col, packed, jnp.where(row < col, -flipped, 0.0))
    scale = jnp.full((1, 1), 1.0, jnp.float32) / (count_ref[0].astype(jnp.float32) * SNAPS)
    top = jnp.concatenate([same, -imag], axis=1) * scale
    square = product(halves(top), halves(whole(top)))
    fourth = product(halves(square), halves(whole(square)))
    power = 2.0 * jnp.sum(fourth * fourth, axis=(0, 1), keepdims=True)
    shift = shift_factor * jnp.sqrt(jnp.sqrt(jnp.sqrt(power)))
    row2 = lax.broadcasted_iota(jnp.int32, (n, 2 * n), 0)
    col2 = lax.broadcasted_iota(jnp.int32, (n, 2 * n), 1)
    shifted = whole(jnp.where(row2 == col2, 1.0, 0.0) - top / shift)
    hi, lo = halves(shifted)
    a_hi[...] = hi
    a_lo[...] = lo
    start_ref[...] = jnp.concatenate([shifted[:NOISE_DIM], shifted[n : n + NOISE_DIM]], axis=0)
    twice = whole(product((hi[:n], lo[:n]), (hi, lo)))
    hi, lo = halves(twice)
    b_hi[...] = hi
    b_lo[...] = lo
    w_ref[...] = jnp.concatenate([twice[:NOISE_DIM], twice[n : n + NOISE_DIM]], axis=0)
    eye = jnp.where(row == col, 1.0, 0.0)

    def steer(piece):
        where = pl.ds(pl.multiple_of(piece * chunk, chunk), chunk)
        position = (grid_ref[:, where].astype(jnp.float32) + 0.5) / OVERSAMPLE
        offset = position - lax.broadcasted_iota(jnp.int32, (n, chunk), 0).astype(jnp.float32)
        angle = (slope * offset) * (slope * offset)
        series = 1.0 / 3.0 + angle * (1.0 / 45.0 + angle * (2.0 / 945.0))
        cot = 1.0 / offset - (slope * slope * offset) * series
        high, low = halves(cot)
        c_hi[:, where] = high
        c_lo[:, where] = low
        length_ref[:, where] = jnp.sum(cot * cot, axis=0, keepdims=True) + n * slope * slope

    def step(coefs, operator=None):
        a, b, c = coefs
        parts = halves(w_ref[...])
        gram = dot_nt(parts[0], parts[0])
        mix = a * eye + b * gram
        if c:
            low = gram.astype(jnp.bfloat16)
            mix = mix + c * dot(low, low)
        moved = halves(product(parts, (operator[0][...], operator[1][...]))) if operator else parts
        w_ref[...] = product_half(halves(mix), moved)

    def distance():
        parts = halves(w_ref[...])
        cross = dot_nt(parts[0], parts[1])
        gram = dot_nt(parts[0], parts[0]) + (cross + dot_nt(parts[1], parts[0]))
        gram_ref[...] = gram
        return jnp.sum((gram - eye) * (gram - eye))

    @pl.loop(0, ITERS // 2 - 1)
    def _(i):
        step(FAST, (b_hi, b_lo))
        steer(2 * i)
        steer(2 * i + 1)

    @pl.loop(ITERS - 2, PIECES)
    def _(i):
        step(FAST)
        steer(i)

    step(CLOSE[0])
    step(CLOSE[1])
    off = distance()

    @pl.when(jnp.logical_not(off < NEAR))
    def _():
        w_ref[...] = start_ref[...]

        @pl.loop(0, ITERS - 1)
        def _(_):
            step(GROW)
            step(CLOSE[0])
            step(CLOSE[1], (a_hi, a_lo))

        step(GROW)
        step(CLOSE[0])
        step(CLOSE[1])
        distance()

    gram = gram_ref[...]
    parts = halves(gram)
    mix = LAST[0] * eye + LAST[1] * gram + LAST[2] * product_half(parts, parts)
    basis = product_half(halves(mix), halves(w_ref[...]))
    bias = -slope * jnp.sum(basis[:, n:], axis=1, keepdims=True)
    lead = halves(basis[:, :n])
    for piece in range(PIECES):
        where = slice(piece * chunk, (piece + 1) * chunk)
        projected = product_half(lead, (c_hi[:, where], c_lo[:, where])) + bias
        energy = jnp.sum(projected * projected, axis=0, keepdims=True)
        out_ref[:, where] = 1.0 / (energy / length_ref[:, where] + spectral_floor)


def finish_user(packed, count, grid_index, beams_total):
    n = WIN_BEAMS
    points = grid_index.shape[1]
    vmem = pl.BlockSpec(memory_space=pltpu.VMEM)
    return pl.pallas_call(
        functools.partial(finish_kernel, beams_total),
        out_shape=jax.ShapeDtypeStruct(grid_index.shape, jnp.float32),
        in_specs=[vmem, pl.BlockSpec(memory_space=pltpu.SMEM), vmem],
        out_specs=vmem,
        scratch_shapes=[
            pltpu.VMEM((2 * n, 2 * n), jnp.bfloat16),
            pltpu.VMEM((2 * n, 2 * n), jnp.bfloat16),
            pltpu.VMEM((2 * n, 2 * n), jnp.bfloat16),
            pltpu.VMEM((2 * n, 2 * n), jnp.bfloat16),
            pltpu.VMEM((n, 2 * n), jnp.float32),
            pltpu.VMEM((n, 2 * n), jnp.float32),
            pltpu.VMEM((n, n), jnp.float32),
            pltpu.VMEM((n, points), jnp.bfloat16),
            pltpu.VMEM((n, points), jnp.bfloat16),
            pltpu.VMEM((1, points), jnp.float32),
        ],
        name="finish_user",
    )(packed, count, grid_index)


def local(beam_data, window_count, slot_owner, slot_window, grid_index):
    owners, groups = lax.axis_size("beam"), lax.axis_size("grp")
    slots = slot_window.shape[1]
    x = beam_data.transpose(0, 2, 1)
    packed = exchange(x, window_count, slot_owner[:, :, 0], slot_window, groups, owners, slots)
    return finish_user(packed, window_count, grid_index, beam_data.shape[1] * owners)


def solution(mesh):
    placed = (
        P(None, "beam", "grp"),
        P(("beam", "grp")),
        P(("beam", "grp"), None, None),
        P(("beam", "grp"), None),
        P(("beam", "grp"), None),
    )
    return jax.shard_map(
        local, mesh=mesh, in_specs=placed, out_specs=P(("beam", "grp"), None), check_vma=False
    )
```

```python
import functools

import jax
import jax.numpy as jnp
from jax import lax
from jax.experimental import pallas as pl
from jax.experimental.pallas import tpu as pltpu
from jax.sharding import PartitionSpec as P

WIN_BEAMS = 128
NOISE_DIM = 64
SNAPS = 256
OVERSAMPLE = 32
ITERS = 8
SIDE = 4
MESH = pl.DeviceIdType.MESH

shift_factor = 1.05
spectral_floor = 0.05


def remote(source, target, send_sem, recv_sem, device):
    return pltpu.make_async_remote_copy(
        src_ref=source,
        dst_ref=target,
        send_sem=send_sem,
        recv_sem=recv_sem,
        device_id=device,
        device_id_type=MESH,
    )


def dot_tn(left, right):
    return lax.dot_general(
        left, right, (((0,), (0,)), ((), ())), preferred_element_type=jnp.float32
    )


def exchange_kernel(
    groups, slots, x_hbm, count_ref, owner_hbm, window_hbm, out_ref, x_ref, owner_ref, window_ref, meta_ref, partial, pieces, metas, chosen, blocks,
    ready, sums, piece_send, piece_recv, meta_send, meta_recv, block_send, block_recv, sum_send, sum_recv, local_sem, load_sem,
):
    b, g = lax.axis_index("beam"), lax.axis_index("grp")
    core, x, y = b % 2, b // (2 * SIDE), (b // 2) % SIDE
    windows, rows = blocks.shape[1:3]

    def along(first, second):
        at_x = (x + first * (1 - core) + second * core) % SIDE
        at_y = (y + first * core + second * (1 - core)) % SIDE
        return (at_x * SIDE + at_y) * 2 + core

    partner = b + 1 - 2 * core
    line = [(g + d) % groups for d in range(groups)]
    order = sorted(range(1, groups), key=lambda d: -min(d, groups - d))
    barrier = pltpu.get_barrier_semaphore()
    greeted = [(b, line[d]) for d in order]
    steps = [(e, d) for e in range(SIDE) for d in range(SIDE) if e or d]
    steps.sort(key=lambda s: -min(s[0], SIDE - s[0]) - min(s[1], SIDE - s[1]))
    greeted += [(along(e, d), g) for e, d in steps]
    greeted += [(partner, g)]
    for device in greeted:
        pl.semaphore_signal(barrier, inc=1, device_id=device, device_id_type=MESH)

    loads = [
        pltpu.make_async_copy(source, target, load_sem.at[i])
        for i, (source, target) in enumerate(
            [(x_hbm, x_ref), (owner_hbm, owner_ref), (window_hbm, window_ref)]
        )
    ]
    for load in loads:
        load.start()
    for load in loads:
        load.wait()
    lane = lax.broadcasted_iota(jnp.int32, meta_ref.shape, 1)
    meta = jnp.full(meta_ref.shape, -1, jnp.int32)
    for k in range(slots):
        wanted = jnp.where(k < count_ref[0], window_ref[0, k], -1)
        meta = jnp.where(lane == k, owner_ref[0, k], jnp.where(lane == slots + k, wanted, meta))
    meta_ref[...] = meta
    row = lax.broadcasted_iota(jnp.int32, (WIN_BEAMS, WIN_BEAMS), 0)
    col = lax.broadcasted_iota(jnp.int32, (WIN_BEAMS, WIN_BEAMS), 1)
    for w in range(windows):
        real = x_ref[0, :, w * WIN_BEAMS : (w + 1) * WIN_BEAMS]
        imag = x_ref[1, :, w * WIN_BEAMS : (w + 1) * WIN_BEAMS]
        same = dot_tn(real, real) + dot_tn(imag, imag)
        cross = dot_tn(imag, real) - dot_tn(real, imag)
        packed = jnp.where(row <= col, same, cross)
        for s in range(groups):
            partial[s, w] = packed[s * rows : (s + 1) * rows]
    pl.semaphore_wait(barrier, len(greeted))

    sent = []

    def send(*args):
        copy = remote(*args)
        copy.start()
        sent.append(copy)

    halves_of = [pl.ds(p * (windows // 2), windows // 2) for p in range(2)]
    for p, part in enumerate(halves_of):
        for d in order:
            target = pieces.at[g, part]
            send(partial.at[line[d], part], target, piece_send.at[p, d], piece_recv.at[p, g], (b, line[d]))
    for d in order:
        send(meta_ref, metas.at[g], meta_send.at[d], meta_recv.at[g], (b, line[d]))
    metas[g] = meta_ref[...]

    count = [0]

    def pass_on(p, block, device):
        piece = blocks.at[block, halves_of[p]]
        send(piece, piece, block_send.at[count[0]], block_recv.at[p, block], (device, g))
        count[0] += 1

    def arrived(p, block):
        piece = blocks.at[block, halves_of[p]]
        remote(piece, piece, block_send.at[0], block_recv.at[p, block], (partner, g)).wait_recv()

    for p, part in enumerate(halves_of):
        own = partial[g, part]
        for d in reversed(order):
            piece = pieces.at[line[d], part]
            remote(piece, piece, piece_send.at[p, d], piece_recv.at[p, line[d]], (b, line[d])).wait_recv()
            own = own + pieces[line[d], part]
        blocks[b, part] = own
        pass_on(p, b, partner)
        for e, d in steps:
            pass_on(p, b, along(e, d))
    for d in range(1, groups):
        remote(meta_ref, metas.at[line[d]], meta_send.at[d], meta_recv.at[line[d]], (b, line[d])).wait_recv()
    fetch = pltpu.make_async_copy(metas, chosen, local_sem)
    fetch.start()
    for p in range(2):
        for e, d in reversed(steps):
            block = along(e, d)
            arrived(p, block)
            pass_on(p, block, partner)
    fetch.wait()
    for p in range(2):
        for i in range(SIDE * SIDE):
            arrived(p, 2 * i + 1 - core)

    for d in order + [0]:
        total = jnp.zeros((rows, WIN_BEAMS), jnp.float32)
        for k in range(slots):
            wanted = chosen[line[d], 0, slots + k]
            weight = jnp.where(wanted >= 0, 1.0, 0.0)
            total = total + weight * blocks[chosen[line[d], 0, k], jnp.maximum(wanted, 0)]
        if d == 0:
            out_ref[g] = total
        else:
            ready[d] = total
            send(ready.at[d], sums.at[g], sum_send.at[d], sum_recv.at[g], (b, line[d]))
    for d in range(1, groups):
        piece = sums.at[line[d]]
        remote(piece, piece, sum_send.at[d], sum_recv.at[line[d]], (b, line[d])).wait_recv()
        out_ref[line[d]] = sums[line[d]]
    for copy in sent:
        copy.wait_send()


def exchange(x, count, owner, window, groups, owners, slots):
    windows, rows = x.shape[2] // WIN_BEAMS, WIN_BEAMS // groups
    vmem, smem = pl.BlockSpec(memory_space=pltpu.VMEM), pl.BlockSpec(memory_space=pltpu.SMEM)
    hbm = pl.BlockSpec(memory_space=pltpu.HBM)
    meta = (8, 128)
    dma = pltpu.SemaphoreType.DMA
    forwards = 2 * (2 * SIDE * SIDE - 1)
    return pl.pallas_call(
        functools.partial(exchange_kernel, groups, slots),
        out_shape=jax.ShapeDtypeStruct((groups, rows, WIN_BEAMS), jnp.float32),
        in_specs=[hbm, smem, hbm, hbm],
        out_specs=vmem,
        scratch_shapes=[
            pltpu.VMEM(x.shape, x.dtype),
            pltpu.SMEM(owner.shape, owner.dtype),
            pltpu.SMEM(window.shape, window.dtype),
            pltpu.VMEM(meta, jnp.int32),
            pltpu.VMEM((groups, windows, rows, WIN_BEAMS), jnp.float32),
            pltpu.VMEM((groups, windows, rows, WIN_BEAMS), jnp.float32),
            pltpu.VMEM((groups,) + meta, jnp.int32),
            pltpu.SMEM((groups,) + meta, jnp.int32),
            pltpu.VMEM((owners, windows, rows, WIN_BEAMS), jnp.float32),
            pltpu.VMEM((groups, rows, WIN_BEAMS), jnp.float32),
            pltpu.VMEM((groups, rows, WIN_BEAMS), jnp.float32),
            dma((2, groups)),
            dma((2, groups)),
            dma((groups,)),
            dma((groups,)),
            dma((forwards,)),
            dma((2, owners)),
            dma((groups,)),
            dma((groups,)),
            dma,
            dma((3,)),
        ],
        compiler_params=pltpu.CompilerParams(collective_id=0, has_side_effects=True),
        name="exchange",
    )(x, count, owner, window).reshape(WIN_BEAMS, WIN_BEAMS)


FAST = (2.4, -1.45, 0.0)
GROW = (3.4445, -4.7750, 2.0315)
CLOSE = ((3.109266, -3.792034, 1.535381), (1.90467, -1.282586, 0.3782733))
LAST = (1.875, -1.25, 0.375)
NEAR = 0.016
PIECES = 8


def halves(value):
    high = value.astype(jnp.bfloat16)
    return high, (value - high.astype(jnp.float32)).astype(jnp.bfloat16)


def dot(left, right):
    return jnp.dot(left, right, preferred_element_type=jnp.float32)


def dot_nt(left, right):
    return lax.dot_general(
        left, right, (((1,), (1,)), ((), ())), preferred_element_type=jnp.float32
    )


def product(left, right):
    return dot(left[0], right[0]) + (dot(left[0], right[1]) + dot(left[1], right[0]))


def product_half(left, right):
    both = dot(
        jnp.concatenate([left[0], left[1]], axis=1),
        jnp.concatenate([right[0], right[0]], axis=0),
    )
    return both + dot(left[0], right[1])


def whole(top):
    n = WIN_BEAMS
    return jnp.concatenate([top, jnp.concatenate([-top[:, n:], top[:, :n]], axis=1)], axis=0)


def finish_kernel(
    beams_total, packed_ref, count_ref, grid_ref, out_ref, a_hi, a_lo, b_hi, b_lo, start_ref, w_ref, gram_ref, c_hi, c_lo, length_ref
):
    n = WIN_BEAMS
    chunk = grid_ref.shape[1] // PIECES
    slope = jnp.pi / beams_total
    row = lax.broadcasted_iota(jnp.int32, (n, n), 0)
    col = lax.broadcasted_iota(jnp.int32, (n, n), 1)
    packed = packed_ref[...]
    flipped = packed.T
    same = jnp.where(row <= col, packed, flipped)
    imag = jnp.where(row > col, packed, jnp.where(row < col, -flipped, 0.0))
    scale = jnp.full((1, 1), 1.0, jnp.float32) / (count_ref[0].astype(jnp.float32) * SNAPS)
    top = jnp.concatenate([same, -imag], axis=1) * scale
    square = product(halves(top), halves(whole(top)))
    fourth = product(halves(square), halves(whole(square)))
    power = 2.0 * jnp.sum(fourth * fourth, axis=(0, 1), keepdims=True)
    shift = shift_factor * jnp.sqrt(jnp.sqrt(jnp.sqrt(power)))
    row2 = lax.broadcasted_iota(jnp.int32, (n, 2 * n), 0)
    col2 = lax.broadcasted_iota(jnp.int32, (n, 2 * n), 1)
    shifted = whole(jnp.where(row2 == col2, 1.0, 0.0) - top / shift)
    hi, lo = halves(shifted)
    a_hi[...] = hi
    a_lo[...] = lo
    start_ref[...] = jnp.concatenate([shifted[:NOISE_DIM], shifted[n : n + NOISE_DIM]], axis=0)
    twice = whole(product((hi[:n], lo[:n]), (hi, lo)))
    hi, lo = halves(twice)
    b_hi[...] = hi
    b_lo[...] = lo
    w_ref[...] = jnp.concatenate([twice[:NOISE_DIM], twice[n : n + NOISE_DIM]], axis=0)
    eye = jnp.where(row == col, 1.0, 0.0)

    def steer(piece):
        where = slice(piece * chunk, (piece + 1) * chunk)
        position = (grid_ref[:, where].astype(jnp.float32) + 0.5) / OVERSAMPLE
        offset = position - lax.broadcasted_iota(jnp.int32, (n, chunk), 0).astype(jnp.float32)
        angle = (slope * offset) * (slope * offset)
        series = 1.0 / 3.0 + angle * (1.0 / 45.0 + angle * (2.0 / 945.0))
        cot = 1.0 / offset - (slope * slope * offset) * series
        high, low = halves(cot)
        c_hi[:, where] = high
        c_lo[:, where] = low
        length_ref[:, where] = jnp.sum(cot * cot, axis=0, keepdims=True) + n * slope * slope

    def step(coefs, operator=None):
        a, b, c = coefs
        parts = halves(w_ref[...])
        gram = dot_nt(parts[0], parts[0])
        mix = a * eye + b * gram
        if c:
            low = gram.astype(jnp.bfloat16)
            mix = mix + c * dot(low, low)
        moved = halves(product(parts, (operator[0][...], operator[1][...]))) if operator else parts
        w_ref[...] = product_half(halves(mix), moved)

    def distance():
        parts = halves(w_ref[...])
        cross = dot_nt(parts[0], parts[1])
        gram = dot_nt(parts[0], parts[0]) + (cross + dot_nt(parts[1], parts[0]))
        gram_ref[...] = gram
        return jnp.sum((gram - eye) * (gram - eye))

    for i in range(ITERS // 2 - 1):
        step(FAST, (b_hi, b_lo))
        steer(2 * i)
        steer(2 * i + 1)

    for i in range(ITERS - 2, PIECES):
        step(FAST)
        steer(i)

    step(CLOSE[0])
    step(CLOSE[1])
    off = distance()

    @pl.when(jnp.logical_not(off < NEAR))
    def _():
        w_ref[...] = start_ref[...]

        @pl.loop(0, ITERS - 1)
        def _(_):
            step(GROW)
            step(CLOSE[0])
            step(CLOSE[1], (a_hi, a_lo))

        step(GROW)
        step(CLOSE[0])
        step(CLOSE[1])
        distance()

    gram = gram_ref[...]
    parts = halves(gram)
    mix = LAST[0] * eye + LAST[1] * gram + LAST[2] * product_half(parts, parts)
    basis = product_half(halves(mix), halves(w_ref[...]))
    bias = -slope * jnp.sum(basis[:, n:], axis=1, keepdims=True)
    lead = halves(basis[:, :n])
    for piece in range(PIECES):
        where = slice(piece * chunk, (piece + 1) * chunk)
        projected = product_half(lead, (c_hi[:, where], c_lo[:, where])) + bias
        energy = jnp.sum(projected * projected, axis=0, keepdims=True)
        out_ref[:, where] = 1.0 / (energy / length_ref[:, where] + spectral_floor)


def finish_user(packed, count, grid_index, beams_total):
    n = WIN_BEAMS
    points = grid_index.shape[1]
    vmem = pl.BlockSpec(memory_space=pltpu.VMEM)
    return pl.pallas_call(
        functools.partial(finish_kernel, beams_total),
        out_shape=jax.ShapeDtypeStruct(grid_index.shape, jnp.float32),
        in_specs=[vmem, pl.BlockSpec(memory_space=pltpu.SMEM), vmem],
        out_specs=vmem,
        scratch_shapes=[
            pltpu.VMEM((2 * n, 2 * n), jnp.bfloat16),
            pltpu.VMEM((2 * n, 2 * n), jnp.bfloat16),
            pltpu.VMEM((2 * n, 2 * n), jnp.bfloat16),
            pltpu.VMEM((2 * n, 2 * n), jnp.bfloat16),
            pltpu.VMEM((n, 2 * n), jnp.float32),
            pltpu.VMEM((n, 2 * n), jnp.float32),
            pltpu.VMEM((n, n), jnp.float32),
            pltpu.VMEM((n, points), jnp.bfloat16),
            pltpu.VMEM((n, points), jnp.bfloat16),
            pltpu.VMEM((1, points), jnp.float32),
        ],
        name="finish_user",
    )(packed, count, grid_index)


def local(beam_data, window_count, slot_owner, slot_window, grid_index):
    owners, groups = lax.axis_size("beam"), lax.axis_size("grp")
    slots = slot_window.shape[1]
    x = beam_data.transpose(0, 2, 1)
    packed = exchange(x, window_count, slot_owner[:, :, 0], slot_window, groups, owners, slots)
    return finish_user(packed, window_count, grid_index, beam_data.shape[1] * owners)


def solution(mesh):
    placed = (
        P(None, "beam", "grp"),
        P(("beam", "grp")),
        P(("beam", "grp"), None, None),
        P(("beam", "grp"), None),
        P(("beam", "grp"), None),
    )
    return jax.shard_map(
        local, mesh=mesh, in_specs=placed, out_specs=P(("beam", "grp"), None), check_vma=False
    )
```

```python
import functools

import jax
import jax.numpy as jnp
from jax import lax
from jax.experimental import pallas as pl
from jax.experimental.pallas import tpu as pltpu
from jax.sharding import PartitionSpec as P

WIN_BEAMS = 128
NOISE_DIM = 64
SNAPS = 256
OVERSAMPLE = 32
ITERS = 8
SIDE = 4
MESH = pl.DeviceIdType.MESH

shift_factor = 1.05
spectral_floor = 0.05


def remote(source, target, send_sem, recv_sem, device):
    return pltpu.make_async_remote_copy(
        src_ref=source,
        dst_ref=target,
        send_sem=send_sem,
        recv_sem=recv_sem,
        device_id=device,
        device_id_type=MESH,
    )


def dot_tn(left, right):
    return lax.dot_general(
        left, right, (((0,), (0,)), ((), ())), preferred_element_type=jnp.float32
    )


def exchange_kernel(
    groups, slots, x_hbm, count_ref, owner_hbm, window_hbm, out_ref, x_ref, owner_ref, window_ref, meta_ref, partial, pieces, metas, chosen, blocks,
    ready, sums, piece_send, piece_recv, meta_send, meta_recv, block_send, block_recv, sum_send, sum_recv, local_sem, load_sem,
):
    b, g = lax.axis_index("beam"), lax.axis_index("grp")
    core, x, y = b % 2, b // (2 * SIDE), (b // 2) % SIDE
    windows, rows = blocks.shape[1:3]

    def along(first, second):
        at_x = (x + first * (1 - core) + second * core) % SIDE
        at_y = (y + first * core + second * (1 - core)) % SIDE
        return (at_x * SIDE + at_y) * 2 + core

    partner = b + 1 - 2 * core
    line = [(g + d) % groups for d in range(groups)]
    order = sorted(range(1, groups), key=lambda d: -min(d, groups - d))
    barrier = pltpu.get_barrier_semaphore()
    greeted = [(b, line[d]) for d in order]
    steps = [(e, d) for e in range(SIDE) for d in range(SIDE) if e or d]
    steps.sort(key=lambda s: -min(s[0], SIDE - s[0]) - min(s[1], SIDE - s[1]))
    greeted += [(along(e, d), g) for e, d in steps]
    greeted += [(partner, g)]
    for device in greeted:
        pl.semaphore_signal(barrier, inc=1, device_id=device, device_id_type=MESH)

    loads = [
        pltpu.make_async_copy(source, target, load_sem.at[i])
        for i, (source, target) in enumerate(
            [(x_hbm, x_ref), (owner_hbm, owner_ref), (window_hbm, window_ref)]
        )
    ]
    for load in loads:
        load.start()
    for load in loads:
        load.wait()
    lane = lax.broadcasted_iota(jnp.int32, meta_ref.shape, 1)
    meta = jnp.full(meta_ref.shape, -1, jnp.int32)
    for k in range(slots):
        wanted = jnp.where(k < count_ref[0], window_ref[0, k], -1)
        meta = jnp.where(lane == k, owner_ref[0, k], jnp.where(lane == slots + k, wanted, meta))
    meta_ref[...] = meta
    row = lax.broadcasted_iota(jnp.int32, (WIN_BEAMS, WIN_BEAMS), 0)
    col = lax.broadcasted_iota(jnp.int32, (WIN_BEAMS, WIN_BEAMS), 1)
    for w in range(windows):
        real = x_ref[0, :, w * WIN_BEAMS : (w + 1) * WIN_BEAMS]
        imag = x_ref[1, :, w * WIN_BEAMS : (w + 1) * WIN_BEAMS]
        same = dot_tn(real, real) + dot_tn(imag, imag)
        cross = dot_tn(imag, real) - dot_tn(real, imag)
        packed = jnp.where(row <= col, same, cross)
        for s in range(groups):
            partial[s, w] = packed[s * rows : (s + 1) * rows]
    pl.semaphore_wait(barrier, len(greeted))

    sent = []

    def send(*args):
        copy = remote(*args)
        copy.start()
        sent.append(copy)

    halves_of = [pl.ds(p * (windows // 2), windows // 2) for p in range(2)]
    for p, part in enumerate(halves_of):
        for d in order:
            target = pieces.at[g, part]
            send(partial.at[line[d], part], target, piece_send.at[p, d], piece_recv.at[p, g], (b, line[d]))
    for d in order:
        send(meta_ref, metas.at[g], meta_send.at[d], meta_recv.at[g], (b, line[d]))
    metas[g] = meta_ref[...]

    count = [0]

    def pass_on(p, block, device):
        piece = blocks.at[block, halves_of[p]]
        send(piece, piece, block_send.at[count[0]], block_recv.at[p, block], (device, g))
        count[0] += 1

    def arrived(p, block):
        piece = blocks.at[block, halves_of[p]]
        remote(piece, piece, block_send.at[0], block_recv.at[p, block], (partner, g)).wait_recv()

    for p, part in enumerate(halves_of):
        own = partial[g, part]
        for d in reversed(order):
            piece = pieces.at[line[d], part]
            remote(piece, piece, piece_send.at[p, d], piece_recv.at[p, line[d]], (b, line[d])).wait_recv()
            own = own + pieces[line[d], part]
        blocks[b, part] = own
        pass_on(p, b, partner)
        for e, d in steps:
            pass_on(p, b, along(e, d))
    for d in range(1, groups):
        remote(meta_ref, metas.at[line[d]], meta_send.at[d], meta_recv.at[line[d]], (b, line[d])).wait_recv()
    fetch = pltpu.make_async_copy(metas, chosen, local_sem)
    fetch.start()
    for p in range(2):
        for e, d in reversed(steps):
            block = along(e, d)
            arrived(p, block)
            pass_on(p, block, partner)
    fetch.wait()
    for p in range(2):
        for i in range(SIDE * SIDE):
            arrived(p, 2 * i + 1 - core)

    for d in order + [0]:
        total = jnp.zeros((rows, WIN_BEAMS), jnp.float32)
        for k in range(slots):
            wanted = chosen[line[d], 0, slots + k]
            weight = jnp.where(wanted >= 0, 1.0, 0.0)
            total = total + weight * blocks[chosen[line[d], 0, k], jnp.maximum(wanted, 0)]
        if d == 0:
            out_ref[g] = total
        else:
            ready[d] = total
            send(ready.at[d], sums.at[g], sum_send.at[d], sum_recv.at[g], (b, line[d]))
    for d in range(1, groups):
        piece = sums.at[line[d]]
        remote(piece, piece, sum_send.at[d], sum_recv.at[line[d]], (b, line[d])).wait_recv()
        out_ref[line[d]] = sums[line[d]]
    for copy in sent:
        copy.wait_send()


def exchange(x, count, owner, window, groups, owners, slots):
    windows, rows = x.shape[2] // WIN_BEAMS, WIN_BEAMS // groups
    vmem, smem = pl.BlockSpec(memory_space=pltpu.VMEM), pl.BlockSpec(memory_space=pltpu.SMEM)
    hbm = pl.BlockSpec(memory_space=pltpu.HBM)
    meta = (8, 128)
    dma = pltpu.SemaphoreType.DMA
    forwards = 2 * (2 * SIDE * SIDE - 1)
    return pl.pallas_call(
        functools.partial(exchange_kernel, groups, slots),
        out_shape=jax.ShapeDtypeStruct((groups, rows, WIN_BEAMS), jnp.float32),
        in_specs=[hbm, smem, hbm, hbm],
        out_specs=vmem,
        scratch_shapes=[
            pltpu.VMEM(x.shape, x.dtype),
            pltpu.SMEM(owner.shape, owner.dtype),
            pltpu.SMEM(window.shape, window.dtype),
            pltpu.VMEM(meta, jnp.int32),
            pltpu.VMEM((groups, windows, rows, WIN_BEAMS), jnp.float32),
            pltpu.VMEM((groups, windows, rows, WIN_BEAMS), jnp.float32),
            pltpu.VMEM((groups,) + meta, jnp.int32),
            pltpu.SMEM((groups,) + meta, jnp.int32),
            pltpu.VMEM((owners, windows, rows, WIN_BEAMS), jnp.float32),
            pltpu.VMEM((groups, rows, WIN_BEAMS), jnp.float32),
            pltpu.VMEM((groups, rows, WIN_BEAMS), jnp.float32),
            dma((2, groups)),
            dma((2, groups)),
            dma((groups,)),
            dma((groups,)),
            dma((forwards,)),
            dma((2, owners)),
            dma((groups,)),
            dma((groups,)),
            dma,
            dma((3,)),
        ],
        compiler_params=pltpu.CompilerParams(collective_id=0, has_side_effects=True),
        name="exchange",
    )(x, count, owner, window).reshape(WIN_BEAMS, WIN_BEAMS)


FAST = (2.4, -1.45, 0.0)
GROW = (3.4445, -4.7750, 2.0315)
CLOSE = ((3.109266, -3.792034, 1.535381), (1.90467, -1.282586, 0.3782733))
LAST = (1.875, -1.25, 0.375)
NEAR = 0.016
PIECES = 8


def halves(value):
    high = value.astype(jnp.bfloat16)
    return high, (value - high.astype(jnp.float32)).astype(jnp.bfloat16)


def dot(left, right):
    return jnp.dot(left, right, preferred_element_type=jnp.float32)


def dot_nt(left, right):
    return lax.dot_general(
        left, right, (((1,), (1,)), ((), ())), preferred_element_type=jnp.float32
    )


def product(left, right):
    return dot(left[0], right[0]) + (dot(left[0], right[1]) + dot(left[1], right[0]))


def product_half(left, right):
    both = dot(
        jnp.concatenate([left[0], left[1]], axis=1),
        jnp.concatenate([right[0], right[0]], axis=0),
    )
    return both + dot(left[0], right[1])


def whole(top):
    n = WIN_BEAMS
    return jnp.concatenate([top, jnp.concatenate([-top[:, n:], top[:, :n]], axis=1)], axis=0)


def finish_kernel(
    beams_total, packed_ref, count_ref, grid_ref, out_ref, a_hi, a_lo, b_hi, b_lo, start_ref, w_ref, gram_ref, c_hi, c_lo, length_ref
):
    n = WIN_BEAMS
    chunk = grid_ref.shape[1] // PIECES
    slope = jnp.pi / beams_total
    row = lax.broadcasted_iota(jnp.int32, (n, n), 0)
    col = lax.broadcasted_iota(jnp.int32, (n, n), 1)
    packed = packed_ref[...]
    flipped = packed.T
    same = jnp.where(row <= col, packed, flipped)
    imag = jnp.where(row > col, packed, jnp.where(row < col, -flipped, 0.0))
    scale = jnp.full((1, 1), 1.0, jnp.float32) / (count_ref[0].astype(jnp.float32) * SNAPS)
    top = jnp.concatenate([same, -imag], axis=1) * scale
    def steer(piece):
        where = slice(piece * chunk, (piece + 1) * chunk)
        position = (grid_ref[:, where].astype(jnp.float32) + 0.5) / OVERSAMPLE
        offset = position - lax.broadcasted_iota(jnp.int32, (n, chunk), 0).astype(jnp.float32)
        angle = (slope * offset) * (slope * offset)
        series = 1.0 / 3.0 + angle * (1.0 / 45.0 + angle * (2.0 / 945.0))
        cot = 1.0 / offset - (slope * slope * offset) * series
        high, low = halves(cot)
        c_hi[:, where] = high
        c_lo[:, where] = low
        length_ref[:, where] = jnp.sum(cot * cot, axis=0, keepdims=True) + n * slope * slope

    square = product(halves(top), halves(whole(top)))
    steer(0)
    steer(1)
    fourth = product(halves(square), halves(whole(square)))
    steer(2)
    power = 2.0 * jnp.sum(fourth * fourth, axis=(0, 1), keepdims=True)
    shift = shift_factor * jnp.sqrt(jnp.sqrt(jnp.sqrt(power)))
    row2 = lax.broadcasted_iota(jnp.int32, (n, 2 * n), 0)
    col2 = lax.broadcasted_iota(jnp.int32, (n, 2 * n), 1)
    shifted = whole(jnp.where(row2 == col2, 1.0, 0.0) - top / shift)
    hi, lo = halves(shifted)
    a_hi[...] = hi
    a_lo[...] = lo
    start_ref[...] = jnp.concatenate([shifted[:NOISE_DIM], shifted[n : n + NOISE_DIM]], axis=0)
    twice = whole(product((hi[:n], lo[:n]), (hi, lo)))
    steer(3)
    hi, lo = halves(twice)
    b_hi[...] = hi
    b_lo[...] = lo
    w_ref[...] = jnp.concatenate([twice[:NOISE_DIM], twice[n : n + NOISE_DIM]], axis=0)
    eye = jnp.where(row == col, 1.0, 0.0)

    def step(coefs, operator=None):
        a, b, c = coefs
        parts = halves(w_ref[...])
        gram = dot_nt(parts[0], parts[0])
        mix = a * eye + b * gram
        if c:
            low = gram.astype(jnp.bfloat16)
            mix = mix + c * dot(low, low)
        moved = halves(product(parts, (operator[0][...], operator[1][...]))) if operator else parts
        w_ref[...] = product_half(halves(mix), moved)

    def distance():
        parts = halves(w_ref[...])
        cross = dot_nt(parts[0], parts[1])
        gram = dot_nt(parts[0], parts[0]) + (cross + dot_nt(parts[1], parts[0]))
        gram_ref[...] = gram
        return jnp.sum((gram - eye) * (gram - eye))

    for i in range(ITERS // 2 - 1):
        step(FAST, (b_hi, b_lo))
        steer(4 + i)

    step(FAST)
    steer(PIECES - 1)
    step(FAST)

    step(CLOSE[0])
    step(CLOSE[1])
    off = distance()

    @pl.when(jnp.logical_not(off < NEAR))
    def _():
        w_ref[...] = start_ref[...]

        @pl.loop(0, ITERS - 1)
        def _(_):
            step(GROW)
            step(CLOSE[0])
            step(CLOSE[1], (a_hi, a_lo))

        step(GROW)
        step(CLOSE[0])
        step(CLOSE[1])
        distance()

    gram = gram_ref[...]
    parts = halves(gram)
    mix = LAST[0] * eye + LAST[1] * gram + LAST[2] * product_half(parts, parts)
    basis = product_half(halves(mix), halves(w_ref[...]))
    bias = -slope * jnp.sum(basis[:, n:], axis=1, keepdims=True)
    lead = halves(basis[:, :n])
    for piece in range(PIECES):
        where = slice(piece * chunk, (piece + 1) * chunk)
        projected = product_half(lead, (c_hi[:, where], c_lo[:, where])) + bias
        energy = jnp.sum(projected * projected, axis=0, keepdims=True)
        out_ref[:, where] = 1.0 / (energy / length_ref[:, where] + spectral_floor)


def finish_user(packed, count, grid_index, beams_total):
    n = WIN_BEAMS
    points = grid_index.shape[1]
    vmem = pl.BlockSpec(memory_space=pltpu.VMEM)
    return pl.pallas_call(
        functools.partial(finish_kernel, beams_total),
        out_shape=jax.ShapeDtypeStruct(grid_index.shape, jnp.float32),
        in_specs=[vmem, pl.BlockSpec(memory_space=pltpu.SMEM), vmem],
        out_specs=vmem,
        scratch_shapes=[
            pltpu.VMEM((2 * n, 2 * n), jnp.bfloat16),
            pltpu.VMEM((2 * n, 2 * n), jnp.bfloat16),
            pltpu.VMEM((2 * n, 2 * n), jnp.bfloat16),
            pltpu.VMEM((2 * n, 2 * n), jnp.bfloat16),
            pltpu.VMEM((n, 2 * n), jnp.float32),
            pltpu.VMEM((n, 2 * n), jnp.float32),
            pltpu.VMEM((n, n), jnp.float32),
            pltpu.VMEM((n, points), jnp.bfloat16),
            pltpu.VMEM((n, points), jnp.bfloat16),
            pltpu.VMEM((1, points), jnp.float32),
        ],
        name="finish_user",
    )(packed, count, grid_index)


def local(beam_data, window_count, slot_owner, slot_window, grid_index):
    owners, groups = lax.axis_size("beam"), lax.axis_size("grp")
    slots = slot_window.shape[1]
    x = beam_data.transpose(0, 2, 1)
    packed = exchange(x, window_count, slot_owner[:, :, 0], slot_window, groups, owners, slots)
    return finish_user(packed, window_count, grid_index, beam_data.shape[1] * owners)


def solution(mesh):
    placed = (
        P(None, "beam", "grp"),
        P(("beam", "grp")),
        P(("beam", "grp"), None, None),
        P(("beam", "grp"), None),
        P(("beam", "grp"), None),
    )
    return jax.shard_map(
        local, mesh=mesh, in_specs=placed, out_specs=P(("beam", "grp"), None), check_vma=False
    )
```
